16 devices in a mesh: dp: 16 (over z, y, x, core).
Axes of the slice: x: 2, y: 2, z: 2, core: 2. Of those that a mesh axis runs over, the one named last changes fastest.
Arguments:
- x_in: bfloat16 [32768, 1024], P('dp')
- dy_mid: bfloat16 [32768, 4096], P('dp')
- x_mid: bfloat16 [32768, 4096], P('dp')
- dy_out: bfloat16 [32768, 1024], P('dp')
- w_fc1: float32 [1024, 4096], replicated
- w_fc2: float32 [4096, 1024], replicated
- stat_left: float32 [32, 512, 512], P('dp')
- stat_right: float32 [32, 512, 512], P('dp')
- root_left: float32 [32, 512, 512], P('dp')
- root_right: float32 [32, 512, 512], P('dp')
- graft_sq: float32 [32, 512, 512], P('dp')
- momentum: float32 [32, 512, 512], P('dp')
Outputs:
- output 1: float32 [1024, 4096], replicated
- output 2: float32 [4096, 1024], replicated
- output 3: float32 [32, 512, 512], P('dp')
- output 4: float32 [32, 512, 512], P('dp')
- output 5: float32 [32, 512, 512], P('dp')
- output 6: float32 [32, 512, 512], P('dp')
All inputs are finite; a program needn't handle non-finite values.
Results may differ from the reference program's by a relative error of at most 0.001.
Values are sent between devices in bfloat16 or wider.
A program may use at most 1 GiB of HBM per device.

```python
import jax
import jax.numpy as jnp

D = 1024
FF = 4096
BLOCK = 512
TOKENS = 2048
DEVICES = 16
STEP = 10

ROW_BLOCKS = (D + BLOCK - 1) // BLOCK
COL_BLOCKS = (FF + BLOCK - 1) // BLOCK
HALF_BLOCKS = ROW_BLOCKS * COL_BLOCKS
NUM_BLOCKS = 2 * HALF_BLOCKS
ROWS_ALL = DEVICES * TOKENS
STAT_DECAY = 0.999
MOM_DECAY = 0.9
GRAFT_EPS = 1e-8
LEARN_RATE = 0.01
WEIGHT_DECAY = 1e-4
BIAS_CORR = 1.0 - STAT_DECAY ** STEP


def spd_draw(key_pair, low_diag, high_diag):
    diag_key, factor_key = jax.random.split(key_pair)
    diag_vals = jax.random.uniform(diag_key, (NUM_BLOCKS, BLOCK), jnp.float32, low_diag, high_diag)
    factor = jax.random.normal(factor_key, (NUM_BLOCKS, BLOCK, 64), jnp.float32)
    low_rank = jnp.einsum('nik,njk->nij', factor, factor) / 128.0
    return low_rank + diag_vals[:, :, None] * jnp.eye(BLOCK, dtype=jnp.float32)


def setup_inputs(seed: int = 0) -> dict:
    key_list = jax.random.split(jax.random.key(seed), 12)
    grad_scale = TOKENS ** -0.5
    stat_scale = 0.01 * BLOCK / DEVICES
    x_in = jax.random.normal(key_list[0], (ROWS_ALL, D), jnp.float32).astype(jnp.bfloat16)
    dy_mid = (jax.random.normal(key_list[1], (ROWS_ALL, FF), jnp.float32) * grad_scale).astype(jnp.bfloat16)
    x_mid = jax.random.normal(key_list[2], (ROWS_ALL, FF), jnp.float32).astype(jnp.bfloat16)
    dy_out = (jax.random.normal(key_list[3], (ROWS_ALL, D), jnp.float32) * grad_scale).astype(jnp.bfloat16)
    w_fc1 = jax.random.normal(key_list[4], (D, FF), jnp.float32) * D ** -0.5
    w_fc2 = jax.random.normal(key_list[5], (FF, D), jnp.float32) * FF ** -0.5
    stat_left = stat_scale * spd_draw(key_list[6], 0.2, 1.0)
    stat_right = stat_scale * spd_draw(key_list[7], 0.2, 1.0)
    root_left = spd_draw(key_list[8], 0.2, 1.0)
    root_right = spd_draw(key_list[9], 0.2, 1.0)
    graft_sq = (BIAS_CORR / DEVICES) * jax.random.uniform(key_list[10], (NUM_BLOCKS, BLOCK, BLOCK), jnp.float32, 0.2, 2.0)
    momentum = jax.random.normal(key_list[11], (NUM_BLOCKS, BLOCK, BLOCK), jnp.float32)
    return {'x_in': x_in, 'dy_mid': dy_mid, 'x_mid': x_mid, 'dy_out': dy_out, 'w_fc1': w_fc1, 'w_fc2': w_fc2, 'stat_left': stat_left, 'stat_right': stat_right, 'root_left': root_left, 'root_right': root_right, 'graft_sq': graft_sq, 'momentum': momentum}


def to_blocks(matrix, row_blocks, col_blocks):
    padded = jnp.pad(matrix, ((0, row_blocks * BLOCK - matrix.shape[0]), (0, col_blocks * BLOCK - matrix.shape[1])))
    return padded.reshape(row_blocks, BLOCK, col_blocks, BLOCK).transpose(0, 2, 1, 3).reshape(row_blocks * col_blocks, BLOCK, BLOCK)


def from_blocks(blocks, row_blocks, col_blocks, n_rows, n_cols):
    full_mat = blocks.reshape(row_blocks, col_blocks, BLOCK, BLOCK).transpose(0, 2, 1, 3)
    return full_mat.reshape(row_blocks * BLOCK, col_blocks * BLOCK)[:n_rows, :n_cols]


def keep_mask(block_ids):
    is_first = block_ids < HALF_BLOCKS
    local_ids = block_ids % HALF_BLOCKS
    row_first = jnp.minimum(D - (local_ids // COL_BLOCKS) * BLOCK, BLOCK)
    col_first = jnp.minimum(FF - (local_ids % COL_BLOCKS) * BLOCK, BLOCK)
    row_second = jnp.minimum(FF - (local_ids // ROW_BLOCKS) * BLOCK, BLOCK)
    col_second = jnp.minimum(D - (local_ids % ROW_BLOCKS) * BLOCK, BLOCK)
    row_count = jnp.where(is_first, row_first, row_second)
    col_count = jnp.where(is_first, col_first, col_second)
    offsets = jnp.arange(BLOCK)
    return (offsets[None, :, None] < row_count[:, None, None]) & (offsets[None, None, :] < col_count[:, None, None])


def reference(x_in, dy_mid, x_mid, dy_out, w_fc1, w_fc2, stat_left, stat_right, root_left, root_right, graft_sq, momentum):
    grad_fc1 = jnp.dot(x_in.T, dy_mid, preferred_element_type=jnp.float32) / DEVICES
    grad_fc2 = jnp.dot(x_mid.T, dy_out, preferred_element_type=jnp.float32) / DEVICES
    grad_blk = jnp.concatenate([to_blocks(grad_fc1, ROW_BLOCKS, COL_BLOCKS), to_blocks(grad_fc2, COL_BLOCKS, ROW_BLOCKS)], axis=0)
    new_left = STAT_DECAY * stat_left + (1.0 - STAT_DECAY) * jnp.einsum('nik,njk->nij', grad_blk, grad_blk)
    new_right = STAT_DECAY * stat_right + (1.0 - STAT_DECAY) * jnp.einsum('nki,nkj->nij', grad_blk, grad_blk)
    precond = jnp.einsum('nij,njk->nik', jnp.einsum('nij,njk->nik', root_left, grad_blk), root_right)
    precond = jnp.where(keep_mask(jnp.arange(NUM_BLOCKS)), precond, 0.0)
    new_sq = STAT_DECAY * graft_sq + (1.0 - STAT_DECAY) * grad_blk * grad_blk
    graft_dir = grad_blk / (jnp.sqrt(new_sq / BIAS_CORR) + GRAFT_EPS)
    graft_norm = jnp.sqrt(jnp.sum(graft_dir * graft_dir, axis=(1, 2)))
    pre_norm = jnp.sqrt(jnp.sum(precond * precond, axis=(1, 2)))
    new_mom = MOM_DECAY * momentum + precond * (graft_norm / pre_norm)[:, None, None]
    direction = new_mom.astype(jnp.bfloat16).astype(jnp.float32)
    dir_fc1 = from_blocks(direction[:HALF_BLOCKS], ROW_BLOCKS, COL_BLOCKS, D, FF)
    dir_fc2 = from_blocks(direction[HALF_BLOCKS:], COL_BLOCKS, ROW_BLOCKS, FF, D)
    new_w1 = w_fc1 - LEARN_RATE * (dir_fc1 + WEIGHT_DECAY * w_fc1)
    new_w2 = w_fc2 - LEARN_RATE * (dir_fc2 + WEIGHT_DECAY * w_fc2)
    return (new_w1, new_w2, new_left, new_right, new_sq, new_mom)
```

```python
import functools

import jax
import jax.numpy as jnp
from jax import lax
from jax.experimental import pallas as pl
from jax.experimental.pallas import tpu as pltpu
from jax.sharding import PartitionSpec as P

STEP = 10
STAT_DECAY = 0.999
MOM_DECAY = 0.9
GRAFT_EPS = 1e-8
LEARN_RATE = 0.01
WEIGHT_DECAY = 1e-4
BIAS_CORR = 1.0 - STAT_DECAY ** STEP

MESH = pl.DeviceIdType.MESH
B = 512
B2 = 2 * B
CH = 32
HALF = B // 2
DEPTH = 4
RING = 8
N_DEV = 16
ORDER = (7, 3, 5, 6, 1, 2, 4, 0)
LANDING = (0, 1, 2, 4, 3, 5, 6, 7)
AXES = ((1, 2, 4), (2, 4, 1), (4, 1, 2))
RS_ROWS = (((0, 176), (176, 168), (344, 168)), ((0, 168), (168, 176), (344, 168)))
AG_ROWS = (((0, 176), (176, 176), (352, 160)), ((0, 160), (160, 176), (336, 176)))
F32 = jnp.float32
BF16 = jnp.bfloat16


def flip(dev, mask):
    out = dev
    for bit in (1, 2, 4):
        if mask & bit:
            width = 2 * bit
            out = out + width - 2 * width * lax.rem(lax.div(dev, width), 2)
    return out


def other_core(dev):
    return dev + 1 - 2 * lax.rem(dev, 2)


def frame_mask(p, m):
    return sum(AXES[p][i] for i in range(3) if m & (1 << i))


def split(v):
    hi = v.astype(BF16)
    return hi, (v - hi.astype(F32)).astype(BF16)


def dot(a, b, ca, cb):
    return lax.dot_general(a, b, (((ca,), (cb,)), ((), ())), preferred_element_type=F32)


def dot_tn(a, b):
    return dot(a, b, 0, 0)


def dot3(a_hi, a_lo, b_hi, b_lo, ca, cb):
    return dot(a_hi, b_hi, ca, cb) + (dot(a_hi, b_lo, ca, cb) + dot(a_lo, b_hi, ca, cb))


def span(t, size):
    return pl.ds(pl.multiple_of(t * size, size), size)


def sweep(fn, init=None):
    def step(t, carry):
        out = fn(span(t, CH), carry)
        return carry if out is None else out

    return lax.fori_loop(0, B // CH, step, jnp.int32(0) if init is None else init)


def bits_of(rel, table, t):
    for n, value in enumerate(table):
        if n:
            rel = jnp.where(t == n, value, rel)
    return rel


def move(dev, rel):
    out = lax.rem(dev, 2)
    for bit in (1, 2, 4):
        out = out + 2 * bit * lax.rem(lax.div(dev, 2 * bit) + lax.div(rel, bit), 2)
    return out


def body(x_in, dy_mid, x_mid, dy_out, w1, w2, st_l, st_r, rt_l, rt_r, gsq, mom,
         w1a, w1b, w2v, o_l, o_r, o_a, o_m, dirs,
         xbuf, ybuf, res, dstage, tbuf, v_l, v_r, v_a, v_m,
         op_sem, st_sem, so_sem, rt_sem, w_sem, own_sem, db_sem, d2d_s, d2d_r, rs_s, rs_r, ag_s, ag_r, dd_s, dd_r, do_s, do_r):
    me = lax.axis_index('dp')
    core = lax.rem(me, 2)
    mate = other_core(me)

    barrier = pltpu.get_barrier_semaphore()
    for nb in (mate, flip(me, 1), flip(me, 2), flip(me, 4)):
        pl.semaphore_signal(barrier, inc=1, device_id=(nb,), device_id_type=MESH)

    def op_start(q):
        h = lax.rem(q, DEPTH)
        side = lax.div(q, DEPTH)
        dest = move(me, bits_of(jnp.int32(ORDER[0]), ORDER, lax.div(side, 2)))
        kd = jnp.where(lax.rem(side, 2) == 0, other_core(dest), dest)
        rows = span(h, B)

        @pl.when(dest < N_DEV // 2)
        def _():
            pltpu.make_async_copy(x_in.at[rows, span(lax.div(kd, 4), B)], xbuf.at[h], op_sem.at[0, h]).start()
            pltpu.make_async_copy(dy_mid.at[rows, span(lax.rem(kd, 4), B2)], ybuf.at[h], op_sem.at[1, h]).start()

        @pl.when(dest >= N_DEV // 2)
        def _():
            pltpu.make_async_copy(x_mid.at[rows, span(kd - N_DEV // 2, B)], xbuf.at[h], op_sem.at[0, h]).start()
            pltpu.make_async_copy(dy_out.at[rows, :], ybuf.at[h], op_sem.at[1, h]).start()

    def op_wait(h):
        pltpu.make_async_copy(x_in.at[pl.ds(0, B), pl.ds(0, B)], xbuf.at[h], op_sem.at[0, h]).wait()
        pltpu.make_async_copy(dy_mid.at[pl.ds(0, B), pl.ds(0, B2)], ybuf.at[h], op_sem.at[1, h]).wait()

    for q in range(DEPTH - 1):
        op_start(jnp.int32(q))
    states = ((st_l, v_l), (st_r, v_r), (gsq, v_a), (mom, v_m))
    for n, (src, dst) in enumerate(states):
        pltpu.make_async_copy(src, dst, st_sem.at[n]).start()
    pl.semaphore_wait(barrier, 4)

    def acc_at(i, r0, rn, c0, cn):
        return (w1a, w1b)[i // 4].at[pl.ds(r0, rn), pl.ds((i % 4) * B2 + c0, cn)]

    def acc_of(rel, s, p):
        r0, rn = RS_ROWS[s][p]
        return acc_at(ORDER.index(rel), r0, rn, s * B, B)

    def got(s, p, j):
        r0, rn = RS_ROWS[s][p]
        return w2v.at[j, pl.ds(r0, rn), pl.ds(s * B, B)]

    def rs_rel(p, j):
        a1, a2, a3 = AXES[p]
        return (a2 | a3, a2, a3, 0, a3, 0, 0)[j]

    def rs_copy(s, p, j):
        axis = AXES[p][0 if j < 4 else (1 if j < 6 else 2)]
        return pltpu.make_async_remote_copy(
            src_ref=acc_of(rs_rel(p, j) | axis, s, p), dst_ref=got(s, p, j),
            send_sem=rs_s.at[s, p, j], recv_sem=rs_r.at[s, p, j],
            device_id=(flip(me, axis),), device_id_type=MESH)

    def rs_take(s, p, j):
        rs_copy(s, p, j).wait_recv()
        ref = acc_of(rs_rel(p, j), s, p)
        ref[...] += got(s, p, j)[...]

    def d2d_copy(i, s, half):
        return pltpu.make_async_remote_copy(
            src_ref=res.at[lax.rem(i, 2), :, pl.ds(s * B, B)], dst_ref=half.at[:, span(lax.rem(i, 4) * 2 + s, B)],
            send_sem=d2d_s.at[s, i], recv_sem=d2d_r.at[s, i], device_id=(mate,), device_id_type=MESH)

    def on_half(i, fn):
        @pl.when(i < 4)
        def _():
            fn(w1a)

        @pl.when(i >= 4)
        def _():
            fn(w1b)

    def compute_step(i, _):
        @pl.when(i >= 2)
        def _():
            for s in range(2):
                d2d_copy(i - 2, s, w1a).wait_send()

        def side(j, _):
            out = jnp.where(j == 0, lax.rem(i, 2), 2)
            for h in range(DEPTH):
                ahead = (i * 2 + j) * DEPTH + h + DEPTH - 1

                @pl.when(ahead < 2 * 8 * DEPTH)
                def _(ahead=ahead):
                    op_start(ahead)
                op_wait(h)
                if h:
                    res[out] += dot_tn(xbuf[h], ybuf[h])
                else:
                    res[out] = dot_tn(xbuf[h], ybuf[h])

            @pl.when(j == 0)
            def _():
                on_half(i, lambda half: [d2d_copy(i, s, half).start() for s in range(2)])
            return 0

        lax.fori_loop(0, 2, side, 0)
        for s in range(2):
            def add_mine(half, s=s):
                d2d_copy(i, s, half).wait_recv()
                cols = span(lax.rem(i, 4) * 2 + s, B)

                def add_rows(rr, _):
                    half[rr, cols] += res[2, rr, pl.ds(s * B, B)]

                sweep(add_rows)

            on_half(i, add_mine)
            for ii in range(7):
                @pl.when(i == ii)
                def _(ii=ii, s=s):
                    for p in range(3):
                        for jj in range(4):
                            if (rs_rel(p, jj) | AXES[p][0]) == ORDER[ii]:
                                rs_copy(s, p, jj).start()
        return 0

    lax.fori_loop(0, 8, compute_step, 0)
    for s in range(2):
        for i in (6, 7):
            d2d_copy(i, s, w1b).wait_send()

    def root_half(s, side):
        return res.at[s, :, pl.ds(side * B, B)]

    for s in range(2):
        for side, src in enumerate((rt_l, rt_r)):
            pltpu.make_async_copy(src.at[s], root_half(s, side), rt_sem.at[s, side]).start()

    def root_hi(s, side):
        return ybuf.at[s, :, pl.ds(side * B, B)]

    def root_lo(s, side):
        return ybuf.at[2 + s, :, pl.ds(side * B, B)]

    def g_hi(s):
        return xbuf.at[s]

    def g_lo(s):
        return xbuf.at[2 + s]

    def prep_roots(s):
        for side, src in enumerate((rt_l, rt_r)):
            pltpu.make_async_copy(src.at[s], root_half(s, side), rt_sem.at[s, side]).wait()

        def rows(rr, _):
            for side in range(2):
                root_hi(s, side)[rr, :], root_lo(s, side)[rr, :] = split(root_half(s, side)[rr, :])

        sweep(rows)

    def state_wait(n):
        pltpu.make_async_copy(states[n][0], states[n][1], st_sem.at[n]).wait()

    def state_out(n):
        return pltpu.make_async_copy(states[n][1], (o_l, o_r, o_a, o_m)[n], so_sem.at[n])

    first_cols = pl.ds(0, B)

    def block_math(s):
        gref = acc_at(ORDER.index(0), 0, B, s * B, B)
        zero = jnp.zeros((8, B), F32)

        def first(rr, tot):
            g = gref[rr, :] * (1.0 / N_DEV)
            g_hi(s)[rr, :], g_lo(s)[rr, :] = split(g)
            sq = STAT_DECAY * v_a[s, rr, :] + (1.0 - STAT_DECAY) * g * g
            v_a[s, rr, :] = sq
            h = g / (jnp.sqrt(sq / BIAS_CORR) + GRAFT_EPS)
            return tot + jnp.sum((h * h).reshape(-1, 8, B), axis=0)

        h_sum = sweep(first, zero)

        def left(t, _):
            rr = span(t, HALF)
            v = dot3(root_hi(s, 0)[rr, :], root_lo(s, 0)[rr, :], g_hi(s)[...], g_lo(s)[...], 1, 0)
            tbuf[0, rr, :], tbuf[1, rr, :] = split(v)
            return 0

        lax.fori_loop(0, 2, left, 0)

        def right(t, tot):
            rr = span(t, HALF)
            v = dot3(tbuf[0, rr, :], tbuf[1, rr, :], root_hi(s, 1)[...], root_lo(s, 1)[...], 1, 0)
            res[2, rr, first_cols] = v
            return tot + jnp.sum((v * v).reshape(-1, 8, B), axis=0)

        p_sum = lax.fori_loop(0, 2, right, zero)
        ratio = jnp.sqrt(jnp.sum(h_sum, keepdims=True)) / jnp.sqrt(jnp.sum(p_sum, keepdims=True))

        def last(rr, _):
            m = MOM_DECAY * v_m[s, rr, :] + res[2, rr, first_cols] * ratio
            v_m[s, rr, :] = m
            dstage[s, rr, :] = m.astype(BF16)

        sweep(last)

    def stats(s):
        hi, lo = g_hi(s), g_lo(s)
        for t in range(2):
            rr = pl.ds(t * HALF, HALF)
            left = dot3(hi[rr, :], lo[rr, :], hi[...], lo[...], 1, 1)
            v_l[s, rr, :] = STAT_DECAY * v_l[s, rr, :] + (1.0 - STAT_DECAY) * left
            right = dot3(hi[:, rr], lo[:, rr], hi[...], lo[...], 0, 0)
            v_r[s, rr, :] = STAT_DECAY * v_r[s, rr, :] + (1.0 - STAT_DECAY) * right

    def rows_of(s, p, blk):
        r0, rn = AG_ROWS[s][p]
        return dirs.at[blk, pl.ds(r0, rn), :]

    def owner(p, m):
        return flip(me, frame_mask(p, m))

    def hi_bit(m):
        return 4 if m & 4 else (2 if m & 2 else 1)

    def ag_copy(s, p, m):
        top = hi_bit(m)
        held = m - top
        r0, rn = AG_ROWS[s][p]
        blk = 2 * owner(p, held) + s
        src = dstage.at[s, pl.ds(r0, rn), :] if held == 0 else rows_of(s, p, blk)
        return pltpu.make_async_remote_copy(
            src_ref=src, dst_ref=rows_of(s, p, blk), send_sem=ag_s.at[s, p, m - 1], recv_sem=ag_r.at[s, p, m - 1],
            device_id=(owner(p, top),), device_id_type=MESH)

    def ag_wait(s, p, m):
        ref = rows_of(s, p, 2 * owner(p, m) + s)
        pltpu.make_async_remote_copy(
            src_ref=ref, dst_ref=ref, send_sem=ag_s.at[s, p, m - 1], recv_sem=ag_r.at[s, p, m - 1],
            device_id=(mate,), device_id_type=MESH).wait_recv()

    def dd_copy(s, p, m):
        ref = rows_of(s, p, 2 * owner(p, m) + s)
        return pltpu.make_async_remote_copy(
            src_ref=ref, dst_ref=ref, send_sem=dd_s.at[s, p, m - 1], recv_sem=dd_r.at[s, p, m - 1],
            device_id=(mate,), device_id_type=MESH)

    def dd_wait(s, p, m):
        ref = rows_of(s, p, 2 * other_core(owner(p, m)) + s)
        pltpu.make_async_remote_copy(
            src_ref=ref, dst_ref=ref, send_sem=dd_s.at[s, p, m - 1], recv_sem=dd_r.at[s, p, m - 1],
            device_id=(mate,), device_id_type=MESH).wait_recv()

    def own_local(s):
        return pltpu.make_async_copy(dstage.at[s], dirs.at[2 * me + s], own_sem.at[s])

    def own_mate(s, recv=False):
        blk = 2 * (mate if recv else me) + s
        return pltpu.make_async_remote_copy(
            src_ref=dstage.at[s], dst_ref=dirs.at[blk], send_sem=do_s.at[s], recv_sem=do_r.at[s],
            device_id=(mate,), device_id_type=MESH)

    def ag_start(s):
        for m in (1, 2, 4):
            for p in range(3):
                ag_copy(s, p, m).start()
        own_mate(s).start()
        own_local(s).start()

    def ag_take(s, ms):
        for m in ms:
            for p in range(3):
                ag_wait(s, p, m)
                for nxt in (2, 4):
                    if nxt > m:
                        ag_copy(s, p, m | nxt).start()
                dd_copy(s, p, m).start()

    for j in range(4):
        for p in range(3):
            rs_take(0, p, j)
            if j < 2:
                rs_copy(0, p, 4 + j).start()
    prep_roots(0)
    prep_roots(1)
    for j in range(4):
        for p in range(3):
            rs_take(1, p, j)
    for p in range(3):
        rs_take(0, p, 4)
        rs_copy(0, p, 6).start()
    for j in range(2):
        for p in range(3):
            rs_copy(1, p, 4 + j).start()
    for j in (5, 6):
        for p in range(3):
            rs_take(0, p, j)
    for n in range(4):
        state_wait(n)
    block_math(0)
    ag_start(0)
    for p in range(3):
        rs_take(1, p, 4)
        rs_copy(1, p, 6).start()
    stats(0)
    for p in range(3):
        rs_take(1, p, 5)
    ag_take(0, (1, 2))
    for p in range(3):
        rs_take(1, p, 6)
    block_math(1)
    ag_start(1)

    for s in range(2):
        for p in range(3):
            for j in range(7):
                rs_copy(s, p, j).wait_send()

    def w_copies():
        out = []
        for n in range(4):
            rr = pl.ds(n * 128, 128)
            out.append(pltpu.make_async_copy(w1.at[rr, :], w1a.at[rr, :], w_sem.at[n]))
            out.append(pltpu.make_async_copy(w1.at[pl.ds(B + n * 128, 128), :], w1b.at[rr, :], w_sem.at[4 + n]))
        for n in range(8):
            out.append(pltpu.make_async_copy(w2.at[pl.ds(n * B, B), :], w2v.at[n], w_sem.at[8 + n]))
        return out

    for cp in w_copies():
        cp.start()
    for n in (2, 3):
        state_out(n).start()
    ag_take(0, (3,))
    stats(1)
    for n in range(2):
        state_out(n).start()

    def ring(slot):
        return ybuf.at[lax.div(slot, 2), :, span(lax.rem(slot, 2), B)]

    def d_load(blk, slot):
        return pltpu.make_async_copy(dirs.at[blk], ring(slot), db_sem.at[slot])

    def apply_rows(out_ref, c, slot):
        cols = span(c, B)

        def rows(rr, _):
            w = out_ref[rr, cols]
            out_ref[rr, cols] = w - LEARN_RATE * (ring(slot)[rr, :].astype(F32) + WEIGHT_DECAY * w)

        sweep(rows)

    def apply_block(blk, slot):
        @pl.when(blk < 8)
        def _():
            apply_rows(w1a, blk, slot)

        @pl.when((blk >= 8) & (blk < N_DEV))
        def _():
            apply_rows(w1b, blk - 8, slot)

        @pl.when(blk >= N_DEV)
        def _():
            apply_rows(w2v.at[lax.div(blk - N_DEV, 2)], lax.rem(blk, 2), slot)

    def apply_range(blk_of, first, last):
        def load(t):
            t = jnp.int32(t)
            return d_load(blk_of(t), lax.rem(t, RING))

        for t in range(first, min(first + RING, last)):
            load(t).start()

        def step(t, _):
            load(t).wait()
            apply_block(blk_of(t), lax.rem(t, RING))

            @pl.when(t + RING < last)
            def _():
                load(t + RING).start()
            return 0

        lax.fori_loop(first, last, step, 0)

    def arriving(dev):
        return lambda t: 2 * move(dev, bits_of(jnp.int32(LANDING[0]), LANDING, t)) + 1

    ag_take(1, (1, 2))
    ag_take(0, (4, 5, 6, 7))
    ag_take(1, (3,))
    for cp in w_copies():
        cp.wait()
    for s in range(2):
        own_local(s).wait()
    own_mate(0, True).wait_recv()
    for m in range(1, 8):
        for p in range(3):
            dd_wait(0, p, m)

    apply_range(lambda t: 2 * t, 0, N_DEV)
    own_mate(1, True).wait_recv()
    apply_range(arriving(me), 0, 1)
    apply_range(arriving(mate), 0, 1)
    for first, last, ms, ds in ((1, 4, (4,), (1, 2, 4)), (4, 7, (5, 6), (3, 5, 6)), (7, 8, (7,), (7,))):
        ag_take(1, ms)
        apply_range(arriving(me), first, last)
        for m in ds:
            for p in range(3):
                dd_wait(1, p, m)
        apply_range(arriving(mate), first, last)
    for n in range(4):
        state_out(n).wait()
    for s in range(2):
        own_mate(s).wait_send()
        for p in range(3):
            for m in range(1, 8):
                ag_copy(s, p, m).wait_send()
                dd_copy(s, p, m).wait_send()


def write_out(w1a, w1b, w2v, ow1, ow2, sem):
    pairs = [(w1a, ow1.at[pl.ds(0, B)]), (w1b, ow1.at[pl.ds(B, B)])]
    pairs += [(w2v.at[n], ow2.at[pl.ds(n * B, B)]) for n in range(8)]
    stores = [pltpu.make_async_copy(src, dst, sem.at[n]) for n, (src, dst) in enumerate(pairs)]
    for cp in stores:
        cp.start()
    for cp in stores:
        cp.wait()


def solution(mesh):
    def per_device(x_in, dy_mid, x_mid, dy_out, w_fc1, w_fc2, stat_left, stat_right, root_left, root_right, graft_sq, momentum):
        vmem = pl.BlockSpec(memory_space=pltpu.VMEM)
        hbm = pl.BlockSpec(memory_space=pltpu.HBM)
        dma = pltpu.SemaphoreType.DMA
        half = pltpu.VMEM((B, w_fc1.shape[1]), F32)
        state = pltpu.HBM(stat_left.shape, F32)
        held = pltpu.VMEM(stat_left.shape, F32)
        tiles = pltpu.VMEM((2, B, B), BF16)
        parts = dma((2, 3, 7))
        pair = dma((2,))
        w1a, w1b, w2v, *states, _ = pl.pallas_call(
            body,
            out_shape=(half, half, pltpu.VMEM((8, B, B2), F32), state, state, state, state, pltpu.HBM((2 * N_DEV, B, B), BF16)),
            in_specs=[hbm] * 12,
            out_specs=(vmem,) * 3 + (hbm,) * 5,
            scratch_shapes=[
                pltpu.VMEM((DEPTH, B, B), BF16), pltpu.VMEM((DEPTH, B, B2), BF16), pltpu.VMEM((3, B, B2), F32), tiles, tiles,
                held, held, held, held, dma((2, DEPTH)), dma((4,)), dma((4,)), dma((2, 2)), dma((16,)), pair, dma((RING,)), dma((2, 8)), dma((2, 8)),
                parts, parts, parts, parts, parts, parts, pair, pair],
            compiler_params=pltpu.CompilerParams(collective_id=0, has_side_effects=True, vmem_limit_bytes=24 << 20),
            name='shampoo_step',
        )(x_in, dy_mid, x_mid, dy_out, w_fc1, w_fc2, stat_left, stat_right, root_left, root_right, graft_sq, momentum)
        new_w1, new_w2 = pl.pallas_call(
            write_out,
            out_shape=(jax.ShapeDtypeStruct(w_fc1.shape, F32), jax.ShapeDtypeStruct(w_fc2.shape, F32)),
            in_specs=[vmem] * 3,
            out_specs=(hbm,) * 2,
            scratch_shapes=[dma((10,))],
            compiler_params=pltpu.CompilerParams(vmem_limit_bytes=1 << 20),
            name='write_out',
        )(w1a, w1b, w2v)
        return (new_w1, new_w2, *states)

    row_spec = P('dp', None)
    rep_spec = P(None, None)
    tile_spec = P('dp', None, None)
    in_specs = (row_spec, row_spec, row_spec, row_spec, rep_spec, rep_spec, tile_spec, tile_spec, tile_spec, tile_spec, tile_spec, tile_spec)
    out_specs = (rep_spec, rep_spec, tile_spec, tile_spec, tile_spec, tile_spec)
    return jax.shard_map(per_device, mesh=mesh, in_specs=in_specs, out_specs=out_specs, check_vma=False)
```

```python
import functools

import jax
import jax.numpy as jnp
from jax import lax
from jax.experimental import pallas as pl
from jax.experimental.pallas import tpu as pltpu
from jax.sharding import PartitionSpec as P

STEP = 10
STAT_DECAY = 0.999
MOM_DECAY = 0.9
GRAFT_EPS = 1e-8
LEARN_RATE = 0.01
WEIGHT_DECAY = 1e-4
BIAS_CORR = 1.0 - STAT_DECAY ** STEP

MESH = pl.DeviceIdType.MESH
B = 512
B2 = 2 * B
CH = 32
HALF = B // 2
DEPTH = 4
RING = 8
VMEM_GRANT = 15 << 20
N_DEV = 16
ORDER = (7, 3, 5, 6, 1, 2, 4, 0)
LANDING = (0, 1, 2, 4, 3, 5, 6, 7)
AXES = ((1, 2, 4), (2, 4, 1), (4, 1, 2))
RS_ROWS = (((0, 176), (176, 168), (344, 168)), ((0, 168), (168, 176), (344, 168)))
AG_ROWS = (((0, 176), (176, 176), (352, 160)), ((0, 160), (160, 176), (336, 176)))
F32 = jnp.float32
BF16 = jnp.bfloat16


def flip(dev, mask):
    out = dev
    for bit in (1, 2, 4):
        if mask & bit:
            width = 2 * bit
            out = out + width - 2 * width * lax.rem(lax.div(dev, width), 2)
    return out


def other_core(dev):
    return dev + 1 - 2 * lax.rem(dev, 2)


def frame_mask(p, m):
    return sum(AXES[p][i] for i in range(3) if m & (1 << i))


def split(v):
    hi = v.astype(BF16)
    return hi, (v - hi.astype(F32)).astype(BF16)


def dot(a, b, ca, cb):
    return lax.dot_general(a, b, (((ca,), (cb,)), ((), ())), preferred_element_type=F32)


def dot_tn(a, b):
    return dot(a, b, 0, 0)


def dot3(a_hi, a_lo, b_hi, b_lo, ca, cb):
    return dot(a_hi, b_hi, ca, cb) + (dot(a_hi, b_lo, ca, cb) + dot(a_lo, b_hi, ca, cb))


def span(t, size):
    return pl.ds(pl.multiple_of(t * size, size), size)


def sweep(fn, init=None):
    def step(t, carry):
        out = fn(span(t, CH), carry)
        return carry if out is None else out

    return lax.fori_loop(0, B // CH, step, jnp.int32(0) if init is None else init)


def bits_of(rel, table, t):
    for n, value in enumerate(table):
        if n:
            rel = jnp.where(t == n, value, rel)
    return rel


def move(dev, rel):
    out = lax.rem(dev, 2)
    for bit in (1, 2, 4):
        out = out + 2 * bit * lax.rem(lax.div(dev, 2 * bit) + lax.div(rel, bit), 2)
    return out


def body(x_in, dy_mid, x_mid, dy_out, w1, w2, st_l, st_r, rt_l, rt_r, gsq, mom,
         w1a, w1b, w2v, v_l, v_r, v_m, kept, dirs,
         xbuf, ybuf, res, dstage, late, v_a,
         op_sem, st_sem, so_sem, rt_sem, w_sem, own_sem, db_sem, d2d_s, d2d_r, rs_s, rs_r, ag_s, ag_r, dd_s, dd_r, do_s, do_r):
    me = lax.axis_index('dp')
    core = lax.rem(me, 2)
    mate = other_core(me)

    barrier = pltpu.get_barrier_semaphore()
    for nb in (mate, flip(me, 1), flip(me, 2), flip(me, 4)):
        pl.semaphore_signal(barrier, inc=1, device_id=(nb,), device_id_type=MESH)

    def op_start(q):
        h = lax.rem(q, DEPTH)
        side = lax.div(q, DEPTH)
        dest = move(me, bits_of(jnp.int32(ORDER[0]), ORDER, lax.div(side, 2)))
        kd = jnp.where(lax.rem(side, 2) == 0, other_core(dest), dest)
        rows = span(h, B)

        @pl.when(dest < N_DEV // 2)
        def _():
            pltpu.make_async_copy(x_in.at[rows, span(lax.div(kd, 4), B)], xbuf.at[h], op_sem.at[0, h]).start()
            pltpu.make_async_copy(dy_mid.at[rows, span(lax.rem(kd, 4), B2)], ybuf.at[h], op_sem.at[1, h]).start()

        @pl.when(dest >= N_DEV // 2)
        def _():
            pltpu.make_async_copy(x_mid.at[rows, span(kd - N_DEV // 2, B)], xbuf.at[h], op_sem.at[0, h]).start()
            pltpu.make_async_copy(dy_out.at[rows, :], ybuf.at[h], op_sem.at[1, h]).start()

    def op_wait(h):
        pltpu.make_async_copy(x_in.at[pl.ds(0, B), pl.ds(0, B)], xbuf.at[h], op_sem.at[0, h]).wait()
        pltpu.make_async_copy(dy_mid.at[pl.ds(0, B), pl.ds(0, B2)], ybuf.at[h], op_sem.at[1, h]).wait()

    for q in range(DEPTH - 1):
        op_start(jnp.int32(q))
    states = ((st_l, v_l), (st_r, v_r), (gsq, v_a), (mom, v_m))
    for n, (src, dst) in enumerate(states):
        pltpu.make_async_copy(src, dst, st_sem.at[n]).start()
    def acc_at(i, r0, rn, c0, cn):
        return (w1a, w1b)[i // 4].at[pl.ds(r0, rn), pl.ds((i % 4) * B2 + c0, cn)]

    def acc_of(rel, s, p):
        r0, rn = RS_ROWS[s][p]
        return acc_at(ORDER.index(rel), r0, rn, s * B, B)

    def got(s, p, j):
        r0, rn = RS_ROWS[s][p]
        return w2v.at[j, pl.ds(r0, rn), pl.ds(s * B, B)]

    def rs_rel(p, j):
        a1, a2, a3 = AXES[p]
        return (a2 | a3, a2, a3, 0, a3, 0, 0)[j]

    def rs_copy(s, p, j):
        axis = AXES[p][0 if j < 4 else (1 if j < 6 else 2)]
        return pltpu.make_async_remote_copy(
            src_ref=acc_of(rs_rel(p, j) | axis, s, p), dst_ref=got(s, p, j),
            send_sem=rs_s.at[s, p, j], recv_sem=rs_r.at[s, p, j],
            device_id=(flip(me, axis),), device_id_type=MESH)

    def rs_take(s, p, j):
        rs_copy(s, p, j).wait_recv()
        ref = acc_of(rs_rel(p, j), s, p)
        ref[...] += got(s, p, j)[...]

    def d2d_copy(i, s, half):
        return pltpu.make_async_remote_copy(
            src_ref=res.at[0, :, pl.ds(s * B, B)], dst_ref=half.at[:, span(lax.rem(i, 4) * 2 + s, B)],
            send_sem=d2d_s.at[s, i], recv_sem=d2d_r.at[s, i], device_id=(mate,), device_id_type=MESH)

    def on_half(i, fn):
        @pl.when(i < 4)
        def _():
            fn(w1a)

        @pl.when(i >= 4)
        def _():
            fn(w1b)

    def compute_step(i, _):
        @pl.when(i >= 1)
        def _():
            for s in range(2):
                d2d_copy(i - 1, s, w1a).wait_send()

        def side(j, _):
            for h in range(DEPTH):
                ahead = (i * 2 + j) * DEPTH + h + DEPTH - 1

                @pl.when(ahead < 2 * 8 * DEPTH)
                def _(ahead=ahead):
                    op_start(ahead)
                op_wait(h)
                if h:
                    res[j] += dot_tn(xbuf[h], ybuf[h])
                else:
                    res[j] = dot_tn(xbuf[h], ybuf[h])

            @pl.when((i == 0) & (j == 0))
            def _():
                pl.semaphore_wait(barrier, 4)

            @pl.when(j == 0)
            def _():
                on_half(i, lambda half: [d2d_copy(i, s, half).start() for s in range(2)])
            return 0

        lax.fori_loop(0, 2, side, 0)
        for s in range(2):
            def add_mine(half, s=s):
                d2d_copy(i, s, half).wait_recv()
                cols = span(lax.rem(i, 4) * 2 + s, B)

                def add_rows(rr, _):
                    half[rr, cols] += res[1, rr, pl.ds(s * B, B)]

                sweep(add_rows)

            on_half(i, add_mine)
            for ii in range(7):
                @pl.when(i == ii)
                def _(ii=ii, s=s):
                    for p in range(3):
                        for jj in range(4):
                            if (rs_rel(p, jj) | AXES[p][0]) == ORDER[ii]:
                                rs_copy(s, p, jj).start()
        return 0

    lax.fori_loop(0, 8, compute_step, 0)
    for s in range(2):
        d2d_copy(7, s, w1b).wait_send()

    def root_half(s, side):
        return res.at[s, :, pl.ds(side * B, B)]

    for s in range(2):
        for side, src in enumerate((rt_l, rt_r)):
            pltpu.make_async_copy(src.at[s], root_half(s, side), rt_sem.at[s, side]).start()

    def root_hi(s, side):
        return ybuf.at[s, :, pl.ds(side * B, B)]

    def root_lo(s, side):
        return ybuf.at[2 + s, :, pl.ds(side * B, B)]

    def g_hi(s):
        return xbuf.at[s]

    def g_lo(s):
        return xbuf.at[2 + s]

    def prep_roots(s):
        for side, src in enumerate((rt_l, rt_r)):
            pltpu.make_async_copy(src.at[s], root_half(s, side), rt_sem.at[s, side]).wait()

        def rows(rr, _):
            for side in range(2):
                root_hi(s, side)[rr, :], root_lo(s, side)[rr, :] = split(root_half(s, side)[rr, :])

        sweep(rows)

    def state_wait(n):
        pltpu.make_async_copy(states[n][0], states[n][1], st_sem.at[n]).wait()

    def square_out():
        return pltpu.make_async_copy(v_a, kept.at[0], so_sem.at[0])

    first_cols = pl.ds(0, B)

    def block_math(s):
        gref = acc_at(ORDER.index(0), 0, B, s * B, B)
        zero = jnp.zeros((8, B), F32)

        def first(rr, tot):
            g = gref[rr, :] * (1.0 / N_DEV)
            g_hi(s)[rr, :], g_lo(s)[rr, :] = split(g)
            sq = STAT_DECAY * v_a[s, rr, :] + (1.0 - STAT_DECAY) * g * g
            v_a[s, rr, :] = sq
            h = g / (jnp.sqrt(sq / BIAS_CORR) + GRAFT_EPS)
            return tot + jnp.sum((h * h).reshape(-1, 8, B), axis=0)

        h_sum = sweep(first, zero)

        def left(t, _):
            rr = span(t, HALF)
            v = dot3(root_hi(s, 0)[rr, :], root_lo(s, 0)[rr, :], g_hi(s)[...], g_lo(s)[...], 1, 0)
            g_hi(1 - s)[rr, :], g_lo(1 - s)[rr, :] = split(v)
            return 0

        lax.fori_loop(0, 2, left, 0)

        def right(t, tot):
            rr = span(t, HALF)
            v = dot3(g_hi(1 - s)[rr, :], g_lo(1 - s)[rr, :], root_hi(s, 1)[...], root_lo(s, 1)[...], 1, 0)
            res[0, rr, first_cols] = v
            return tot + jnp.sum((v * v).reshape(-1, 8, B), axis=0)

        p_sum = lax.fori_loop(0, 2, right, zero)
        ratio = jnp.sqrt(jnp.sum(h_sum, keepdims=True)) / jnp.sqrt(jnp.sum(p_sum, keepdims=True))

        def last(rr, _):
            m = MOM_DECAY * v_m[s, rr, :] + res[0, rr, first_cols] * ratio
            v_m[s, rr, :] = m
            dstage[s, rr, :] = m.astype(BF16)

        sweep(last)

    def stats(s):
        hi, lo = g_hi(s), g_lo(s)
        for t in range(2):
            rr = pl.ds(t * HALF, HALF)
            left = dot3(hi[rr, :], lo[rr, :], hi[...], lo[...], 1, 1)
            v_l[s, rr, :] = STAT_DECAY * v_l[s, rr, :] + (1.0 - STAT_DECAY) * left
            right = dot3(hi[:, rr], lo[:, rr], hi[...], lo[...], 0, 0)
            v_r[s, rr, :] = STAT_DECAY * v_r[s, rr, :] + (1.0 - STAT_DECAY) * right

    def rows_of(s, p, blk):
        r0, rn = AG_ROWS[s][p]
        return dirs.at[blk, pl.ds(r0, rn), :]

    def owner(p, m):
        return flip(me, frame_mask(p, m))

    def hi_bit(m):
        return 4 if m & 4 else (2 if m & 2 else 1)

    def landing(s, p, m, core_of=0):
        if s == 1 and m == 7:
            r0, rn = AG_ROWS[s][p]
            return late.at[core_of, pl.ds(r0, rn), :]
        dev = owner(p, m)
        return rows_of(s, p, 2 * (other_core(dev) if core_of else dev) + s)

    def ag_copy(s, p, m):
        top = hi_bit(m)
        held = m - top
        r0, rn = AG_ROWS[s][p]
        blk = 2 * owner(p, held) + s
        src = dstage.at[s, pl.ds(r0, rn), :] if held == 0 else rows_of(s, p, blk)
        dst = landing(s, p, m) if m == 7 and s == 1 else rows_of(s, p, blk)
        return pltpu.make_async_remote_copy(
            src_ref=src, dst_ref=dst, send_sem=ag_s.at[s, p, m - 1], recv_sem=ag_r.at[s, p, m - 1],
            device_id=(owner(p, top),), device_id_type=MESH)

    def ag_wait(s, p, m):
        ref = landing(s, p, m)
        pltpu.make_async_remote_copy(
            src_ref=ref, dst_ref=ref, send_sem=ag_s.at[s, p, m - 1], recv_sem=ag_r.at[s, p, m - 1],
            device_id=(mate,), device_id_type=MESH).wait_recv()

    def dd_copy(s, p, m):
        ref = landing(s, p, m)
        return pltpu.make_async_remote_copy(
            src_ref=ref, dst_ref=landing(s, p, m, 1) if m == 7 and s == 1 else ref,
            send_sem=dd_s.at[s, p, m - 1], recv_sem=dd_r.at[s, p, m - 1],
            device_id=(mate,), device_id_type=MESH)

    def dd_wait(s, ms):
        for m in ms:
            for p in range(3):
                ref = landing(s, p, m, 1)
                pltpu.make_async_remote_copy(
                    src_ref=ref, dst_ref=ref, send_sem=dd_s.at[s, p, m - 1], recv_sem=dd_r.at[s, p, m - 1],
                    device_id=(mate,), device_id_type=MESH).wait_recv()

    def own_local(s):
        return pltpu.make_async_copy(dstage.at[s], dirs.at[2 * me + s], own_sem.at[s])

    def own_mate(s, recv=False):
        blk = 2 * (mate if recv else me) + s
        return pltpu.make_async_remote_copy(
            src_ref=dstage.at[s], dst_ref=dirs.at[blk], send_sem=do_s.at[s], recv_sem=do_r.at[s],
            device_id=(mate,), device_id_type=MESH)

    def ag_start(s):
        for m in (1, 2, 4):
            for p in range(3):
                ag_copy(s, p, m).start()
        own_mate(s).start()
        own_local(s).start()

    def ag_take(s, ms):
        for m in ms:
            for p in range(3):
                ag_wait(s, p, m)
                for nxt in (2, 4):
                    if nxt > m:
                        ag_copy(s, p, m | nxt).start()
                dd_copy(s, p, m).start()

    for j in range(4):
        for p in range(3):
            rs_take(0, p, j)
            if j < 2:
                rs_copy(0, p, 4 + j).start()
    prep_roots(0)
    prep_roots(1)
    for j in range(4):
        for p in range(3):
            rs_take(1, p, j)
    for p in range(3):
        rs_take(0, p, 4)
        rs_copy(0, p, 6).start()
    for j in range(2):
        for p in range(3):
            rs_copy(1, p, 4 + j).start()
    for j in (5, 6):
        for p in range(3):
            rs_take(0, p, j)
    for n in range(4):
        state_wait(n)
    block_math(0)
    ag_start(0)
    for p in range(3):
        rs_take(1, p, 4)
        rs_copy(1, p, 6).start()
    stats(0)
    for p in range(3):
        rs_take(1, p, 5)
    ag_take(0, (1, 2))
    for p in range(3):
        rs_take(1, p, 6)
    block_math(1)
    ag_start(1)

    for s in range(2):
        for p in range(3):
            for j in range(7):
                rs_copy(s, p, j).wait_send()

    def w_copies():
        out = []
        for n in range(4):
            rr = pl.ds(n * 128, 128)
            out.append(pltpu.make_async_copy(w1.at[rr, :], w1a.at[rr, :], w_sem.at[n]))
            out.append(pltpu.make_async_copy(w1.at[pl.ds(B + n * 128, 128), :], w1b.at[rr, :], w_sem.at[4 + n]))
        for n in range(8):
            out.append(pltpu.make_async_copy(w2.at[pl.ds(n * B, B), :], w2v.at[n], w_sem.at[8 + n]))
        return out

    for cp in w_copies():
        cp.start()
    square_out().start()
    ag_take(0, (3,))
    stats(1)

    def ring(slot):
        return ybuf.at[lax.div(slot, 2), :, span(lax.rem(slot, 2), B)]

    def d_load(blk, slot):
        return pltpu.make_async_copy(dirs.at[blk], ring(slot), db_sem.at[slot])

    def apply_rows(out_ref, c, src):
        cols = span(c, B)

        def rows(rr, _):
            w = out_ref[rr, cols]
            out_ref[rr, cols] = w - LEARN_RATE * (src[rr, :].astype(F32) + WEIGHT_DECAY * w)

        sweep(rows)

    def apply_block(blk, src):
        @pl.when(blk < 8)
        def _():
            apply_rows(w1a, blk, src)

        @pl.when((blk >= 8) & (blk < N_DEV))
        def _():
            apply_rows(w1b, blk - 8, src)

        @pl.when(blk >= N_DEV)
        def _():
            apply_rows(w2v.at[lax.div(blk - N_DEV, 2)], lax.rem(blk, 2), src)

    def apply_range(blk_of, first, last):
        def load(t):
            t = jnp.int32(t)
            return d_load(blk_of(t), lax.rem(t, RING))

        for t in range(first, min(first + RING, last)):
            load(t).start()

        def step(t, _):
            load(t).wait()
            apply_block(blk_of(t), ring(lax.rem(t, RING)))

            @pl.when(t + RING < last)
            def _():
                load(t + RING).start()
            return 0

        lax.fori_loop(first, last, step, 0)

    def arriving(dev, s):
        return lambda t: 2 * move(dev, bits_of(jnp.int32(LANDING[0]), LANDING, t)) + s

    def sent(s, ms):
        for p in range(3):
            for m in ms:
                ag_copy(s, p, m).wait_send()
                dd_copy(s, p, m).wait_send()

    ag_take(1, (1, 2))
    for cp in w_copies():
        cp.wait()
    for s in range(2):
        own_local(s).wait()
        own_mate(s).wait_send()
        own_mate(s, True).wait_recv()
    ag_take(0, (4, 5, 6))
    apply_range(arriving(me, 0), 0, 7)
    dd_wait(0, range(1, 7))
    apply_range(arriving(mate, 0), 0, 7)
    ag_take(0, (7,))
    apply_range(arriving(me, 0), 7, 8)
    apply_range(arriving(me, 1), 0, 1)
    ag_take(1, (3,))
    sent(0, range(1, 8))
    dd_wait(0, (7,))
    apply_range(arriving(mate, 0), 7, 8)
    apply_range(arriving(mate, 1), 0, 1)
    ag_take(1, (4,))
    apply_range(arriving(me, 1), 1, 4)
    ag_take(1, (5, 6))
    dd_wait(1, (1, 2, 4))
    apply_range(arriving(mate, 1), 1, 4)
    apply_range(arriving(me, 1), 4, 7)
    dd_wait(1, (3, 5, 6))
    apply_range(arriving(mate, 1), 4, 7)
    sent(1, range(1, 7))
    square_out().wait()
    ag_take(1, (7,))
    apply_block(arriving(me, 1)(7), late.at[0])
    dd_wait(1, (7,))
    apply_block(arriving(mate, 1)(7), late.at[1])
    sent(1, (7,))


def write_out(w1a, w1b, w2v, v_l, v_r, v_m, kept, ow1, ow2, o_l, o_r, o_a, o_m, v_a, in_sem, sem):
    load = pltpu.make_async_copy(kept.at[0], v_a, in_sem.at[0])
    pairs = [(v_a, o_a), (v_l, o_l), (v_r, o_r), (v_m, o_m), (w1a, ow1.at[pl.ds(0, B)]), (w1b, ow1.at[pl.ds(B, B)])]
    pairs += [(w2v.at[n], ow2.at[pl.ds(n * B, B)]) for n in range(8)]
    stores = [pltpu.make_async_copy(src, dst, sem.at[n]) for n, (src, dst) in enumerate(pairs)]
    for cp in [load] + stores[1:]:
        cp.start()
    load.wait()
    for cp in stores[:1]:
        cp.start()
    for cp in stores:
        cp.wait()


def solution(mesh):
    def per_device(x_in, dy_mid, x_mid, dy_out, w_fc1, w_fc2, stat_left, stat_right, root_left, root_right, graft_sq, momentum):
        vmem = pl.BlockSpec(memory_space=pltpu.VMEM)
        hbm = pl.BlockSpec(memory_space=pltpu.HBM)
        dma = pltpu.SemaphoreType.DMA
        half = pltpu.VMEM((B, w_fc1.shape[1]), F32)
        kept = pltpu.HBM((N_DEV,) + stat_left.shape, F32)
        state = held = pltpu.VMEM(stat_left.shape, F32)
        tiles = pltpu.VMEM((2, B, B), BF16)
        parts = dma((2, 3, 7))
        pair = dma((2,))
        *done, _ = pl.pallas_call(
            body,
            out_shape=(half, half, pltpu.VMEM((8, B, B2), F32), state, state, state, kept, pltpu.HBM((2 * N_DEV, B, B), BF16)),
            in_specs=[hbm] * 12,
            out_specs=(vmem,) * 6 + (hbm,) * 2,
            scratch_shapes=[
                pltpu.VMEM((DEPTH, B, B), BF16), pltpu.VMEM((DEPTH, B, B2), BF16), pltpu.VMEM((2, B, B2), F32), tiles, tiles, held,
                dma((2, DEPTH)), dma((4,)), dma((1,)), dma((2, 2)), dma((16,)), pair, dma((RING,)), dma((2, 8)), dma((2, 8)),
                parts, parts, parts, parts, parts, parts, pair, pair],
            compiler_params=pltpu.CompilerParams(collective_id=0, has_side_effects=True, vmem_limit_bytes=VMEM_GRANT),
            name='shampoo_step',
        )(x_in, dy_mid, x_mid, dy_out, w_fc1, w_fc2, stat_left, stat_right, root_left, root_right, graft_sq, momentum)
        like = (w_fc1, w_fc2, stat_left, stat_right, graft_sq, momentum)
        return pl.pallas_call(
            write_out,
            out_shape=tuple(jax.ShapeDtypeStruct(v.shape, F32) for v in like),
            in_specs=[vmem] * 6 + [hbm],
            out_specs=(hbm,) * 6,
            scratch_shapes=[held, dma((1,)), dma((14,))],
            compiler_params=pltpu.CompilerParams(vmem_limit_bytes=VMEM_GRANT),
            name='write_out',
        )(*done)

    row_spec = P('dp', None)
    rep_spec = P(None, None)
    tile_spec = P('dp', None, None)
    in_specs = (row_spec, row_spec, row_spec, row_spec, rep_spec, rep_spec, tile_spec, tile_spec, tile_spec, tile_spec, tile_spec, tile_spec)
    out_specs = (rep_spec, rep_spec, tile_spec, tile_spec, tile_spec, tile_spec)
    return jax.shard_map(per_device, mesh=mesh, in_specs=in_specs, out_specs=out_specs, check_vma=False)
```

```python
import functools

import jax
import jax.numpy as jnp
from jax import lax
from jax.experimental import pallas as pl
from jax.experimental.pallas import tpu as pltpu
from jax.sharding import PartitionSpec as P

STEP = 10
STAT_DECAY = 0.999
MOM_DECAY = 0.9
GRAFT_EPS = 1e-8
LEARN_RATE = 0.01
WEIGHT_DECAY = 1e-4
BIAS_CORR = 1.0 - STAT_DECAY ** STEP

MESH = pl.DeviceIdType.MESH
B = 512
B2 = 2 * B
CH = 32
HALF = B // 2
DEPTH = 4
RING = 8
VMEM_GRANT = 15 << 20
N_DEV = 16
ORDER = (7, 3, 5, 6, 1, 2, 4, 0)
LANDING = (0, 1, 2, 4, 3, 5, 6, 7)
AXES = ((1, 2, 4), (2, 4, 1), (4, 1, 2))
RS_ROWS = (((0, 176), (176, 168), (344, 168)), ((0, 168), (168, 176), (344, 168)))
AG_ROWS = (((0, 176), (176, 176), (352, 160)), ((0, 160), (160, 176), (336, 176)))
F32 = jnp.float32
BF16 = jnp.bfloat16


def flip(dev, mask):
    out = dev
    for bit in (1, 2, 4):
        if mask & bit:
            width = 2 * bit
            out = out + width - 2 * width * lax.rem(lax.div(dev, width), 2)
    return out


def other_core(dev):
    return dev + 1 - 2 * lax.rem(dev, 2)


def frame_mask(p, m):
    return sum(AXES[p][i] for i in range(3) if m & (1 << i))


def split(v):
    hi = v.astype(BF16)
    return hi, (v - hi.astype(F32)).astype(BF16)


def dot(a, b, ca, cb):
    return lax.dot_general(a, b, (((ca,), (cb,)), ((), ())), preferred_element_type=F32)


def dot_tn(a, b):
    return dot(a, b, 0, 0)


def dot3(a_hi, a_lo, b_hi, b_lo, ca, cb):
    return dot(a_hi, b_hi, ca, cb) + (dot(a_hi, b_lo, ca, cb) + dot(a_lo, b_hi, ca, cb))


def span(t, size):
    return pl.ds(pl.multiple_of(t * size, size), size)


def sweep(fn, init=None):
    def step(t, carry):
        out = fn(span(t, CH), carry)
        return carry if out is None else out

    return lax.fori_loop(0, B // CH, step, jnp.int32(0) if init is None else init)


def bits_of(rel, table, t):
    for n, value in enumerate(table):
        if n:
            rel = jnp.where(t == n, value, rel)
    return rel


def move(dev, rel):
    out = lax.rem(dev, 2)
    for bit in (1, 2, 4):
        out = out + 2 * bit * lax.rem(lax.div(dev, 2 * bit) + lax.div(rel, bit), 2)
    return out


def body(x_in, dy_mid, x_mid, dy_out, w1, w2, st_l, st_r, rt_l, rt_r, gsq, mom,
         w1a, w1b, w2v, v_l, v_r, v_m, kept, dirs,
         xbuf, ybuf, res, dstage, late, v_a,
         op_sem, st_sem, so_sem, rt_sem, w_sem, own_sem, db_sem, d2d_s, d2d_r, rs_s, rs_r, ag_s, ag_r, dd_s, dd_r, do_s, do_r):
    me = lax.axis_index('dp')
    core = lax.rem(me, 2)
    mate = other_core(me)

    barrier = pltpu.get_barrier_semaphore()
    for nb in (mate, flip(me, 1), flip(me, 2), flip(me, 4)):
        pl.semaphore_signal(barrier, inc=1, device_id=(nb,), device_id_type=MESH)

    def op_start(q):
        h = lax.rem(q, DEPTH)
        side = lax.div(q, DEPTH)
        dest = move(me, bits_of(jnp.int32(ORDER[0]), ORDER, lax.div(side, 2)))
        kd = jnp.where(lax.rem(side, 2) == 0, other_core(dest), dest)
        rows = span(h, B)

        @pl.when(dest < N_DEV // 2)
        def _():
            pltpu.make_async_copy(x_in.at[rows, span(lax.div(kd, 4), B)], xbuf.at[h], op_sem.at[0, h]).start()
            pltpu.make_async_copy(dy_mid.at[rows, span(lax.rem(kd, 4), B2)], ybuf.at[h], op_sem.at[1, h]).start()

        @pl.when(dest >= N_DEV // 2)
        def _():
            pltpu.make_async_copy(x_mid.at[rows, span(kd - N_DEV // 2, B)], xbuf.at[h], op_sem.at[0, h]).start()
            pltpu.make_async_copy(dy_out.at[rows, :], ybuf.at[h], op_sem.at[1, h]).start()

    def op_wait(h):
        pltpu.make_async_copy(x_in.at[pl.ds(0, B), pl.ds(0, B)], xbuf.at[h], op_sem.at[0, h]).wait()
        pltpu.make_async_copy(dy_mid.at[pl.ds(0, B), pl.ds(0, B2)], ybuf.at[h], op_sem.at[1, h]).wait()

    for q in range(DEPTH - 1):
        op_start(jnp.int32(q))
    states = ((st_l, v_l), (st_r, v_r), (gsq, v_a), (mom, v_m))
    def acc_at(i, r0, rn, c0, cn):
        return (w1a, w1b)[i // 4].at[pl.ds(r0, rn), pl.ds((i % 4) * B2 + c0, cn)]

    def acc_of(rel, s, p):
        r0, rn = RS_ROWS[s][p]
        return acc_at(ORDER.index(rel), r0, rn, s * B, B)

    def got(s, p, j):
        r0, rn = RS_ROWS[s][p]
        return w2v.at[j, pl.ds(r0, rn), pl.ds(s * B, B)]

    def rs_rel(p, j):
        a1, a2, a3 = AXES[p]
        return (a2 | a3, a2, a3, 0, a3, 0, 0)[j]

    def rs_copy(s, p, j):
        axis = AXES[p][0 if j < 4 else (1 if j < 6 else 2)]
        return pltpu.make_async_remote_copy(
            src_ref=acc_of(rs_rel(p, j) | axis, s, p), dst_ref=got(s, p, j),
            send_sem=rs_s.at[0], recv_sem=rs_r.at[s, j],
            device_id=(flip(me, axis),), device_id_type=MESH)

    def wait_all(ref, send_sem, recv_sem):
        return pltpu.make_async_remote_copy(
            src_ref=ref, dst_ref=ref, send_sem=send_sem, recv_sem=recv_sem, device_id=(mate,), device_id_type=MESH)

    def rs_take(s, j, then=()):
        wait_all(w2v.at[j, :, pl.ds(s * B, B)], rs_s.at[0], rs_r.at[s, j]).wait_recv()
        for p in range(3):
            ref = acc_of(rs_rel(p, j), s, p)
            ref[...] += got(s, p, j)[...]
            for nxt in then:
                rs_copy(s, p, nxt).start()

    def d2d_copy(i, s, half):
        return pltpu.make_async_remote_copy(
            src_ref=res.at[0, :, pl.ds(s * B, B)], dst_ref=half.at[:, span(lax.rem(i, 4) * 2 + s, B)],
            send_sem=d2d_s.at[0], recv_sem=d2d_r.at[s, lax.rem(i, 2)], device_id=(mate,), device_id_type=MESH)

    def on_half(i, fn):
        @pl.when(i < 4)
        def _():
            fn(w1a)

        @pl.when(i >= 4)
        def _():
            fn(w1b)

    def compute_step(i, _):
        @pl.when(i >= 1)
        def _():
            wait_all(res.at[0], d2d_s.at[0], d2d_r.at[0, 0]).wait_send()

        def side(j, _):
            for h in range(DEPTH):
                ahead = (i * 2 + j) * DEPTH + h + DEPTH - 1

                @pl.when(ahead < 2 * 8 * DEPTH)
                def _(ahead=ahead):
                    op_start(ahead)
                op_wait(h)
                if h:
                    res[j] += dot_tn(xbuf[h], ybuf[h])
                else:
                    res[j] = dot_tn(xbuf[h], ybuf[h])

            @pl.when((i == 0) & (j == 0))
            def _():
                pl.semaphore_wait(barrier, 4)

            @pl.when(j == 0)
            def _():
                on_half(i, lambda half: [d2d_copy(i, s, half).start() for s in range(2)])
            return 0

        lax.fori_loop(0, 2, side, 0)
        for s in range(2):
            def add_mine(half, s=s):
                d2d_copy(i, s, half).wait_recv()
                cols = span(lax.rem(i, 4) * 2 + s, B)

                def add_rows(rr, _):
                    half[rr, cols] += res[1, rr, pl.ds(s * B, B)]

                sweep(add_rows)

            on_half(i, add_mine)
            for ii in range(7):
                @pl.when(i == ii)
                def _(ii=ii, s=s):
                    for p in range(3):
                        for jj in range(4):
                            if (rs_rel(p, jj) | AXES[p][0]) == ORDER[ii]:
                                rs_copy(s, p, jj).start()
        return 0

    lax.fori_loop(0, 8, compute_step, 0)
    wait_all(res.at[0], d2d_s.at[0], d2d_r.at[0, 0]).wait_send()

    for n, (src, dst) in enumerate(states):
        pltpu.make_async_copy(src, dst, st_sem.at[n]).start()

    def root_half(s, side):
        return res.at[s, :, pl.ds(side * B, B)]

    for s in range(2):
        for side, src in enumerate((rt_l, rt_r)):
            pltpu.make_async_copy(src.at[s], root_half(s, side), rt_sem.at[s, side]).start()

    def root_hi(s, side):
        return ybuf.at[s, :, pl.ds(side * B, B)]

    def root_lo(s, side):
        return ybuf.at[2 + s, :, pl.ds(side * B, B)]

    def g_hi(s):
        return xbuf.at[s]

    def g_lo(s):
        return xbuf.at[2 + s]

    def prep_roots(s):
        for side, src in enumerate((rt_l, rt_r)):
            pltpu.make_async_copy(src.at[s], root_half(s, side), rt_sem.at[s, side]).wait()

        def rows(rr, _):
            for side in range(2):
                root_hi(s, side)[rr, :], root_lo(s, side)[rr, :] = split(root_half(s, side)[rr, :])

        sweep(rows)

    def state_wait(n):
        pltpu.make_async_copy(states[n][0], states[n][1], st_sem.at[n]).wait()

    def square_out():
        return pltpu.make_async_copy(v_a, kept.at[0], so_sem.at[0])

    first_cols = pl.ds(0, B)

    def block_math(s):
        gref = acc_at(ORDER.index(0), 0, B, s * B, B)
        zero = jnp.zeros((8, B), F32)

        def first(rr, tot):
            g = gref[rr, :] * (1.0 / N_DEV)
            g_hi(s)[rr, :], g_lo(s)[rr, :] = split(g)
            sq = STAT_DECAY * v_a[s, rr, :] + (1.0 - STAT_DECAY) * g * g
            v_a[s, rr, :] = sq
            h = g / (jnp.sqrt(sq / BIAS_CORR) + GRAFT_EPS)
            return tot + jnp.sum((h * h).reshape(-1, 8, B), axis=0)

        h_sum = sweep(first, zero)

        def left(t, _):
            rr = span(t, HALF)
            v = dot3(root_hi(s, 0)[rr, :], root_lo(s, 0)[rr, :], g_hi(s)[...], g_lo(s)[...], 1, 0)
            g_hi(1 - s)[rr, :], g_lo(1 - s)[rr, :] = split(v)
            return 0

        lax.fori_loop(0, 2, left, 0)

        def right(t, tot):
            rr = span(t, HALF)
            v = dot3(g_hi(1 - s)[rr, :], g_lo(1 - s)[rr, :], root_hi(s, 1)[...], root_lo(s, 1)[...], 1, 0)
            res[0, rr, first_cols] = v
            return tot + jnp.sum((v * v).reshape(-1, 8, B), axis=0)

        p_sum = lax.fori_loop(0, 2, right, zero)
        ratio = jnp.sqrt(jnp.sum(h_sum, keepdims=True)) / jnp.sqrt(jnp.sum(p_sum, keepdims=True))

        def last(rr, _):
            m = MOM_DECAY * v_m[s, rr, :] + res[0, rr, first_cols] * ratio
            v_m[s, rr, :] = m
            dstage[s, rr, :] = m.astype(BF16)

        sweep(last)

    def stats(s):
        hi, lo = g_hi(s), g_lo(s)
        for t in range(2):
            rr = pl.ds(t * HALF, HALF)
            left = dot3(hi[rr, :], lo[rr, :], hi[...], lo[...], 1, 1)
            v_l[s, rr, :] = STAT_DECAY * v_l[s, rr, :] + (1.0 - STAT_DECAY) * left
            right = dot3(hi[:, rr], lo[:, rr], hi[...], lo[...], 0, 0)
            v_r[s, rr, :] = STAT_DECAY * v_r[s, rr, :] + (1.0 - STAT_DECAY) * right

    def rows_of(s, p, blk):
        r0, rn = AG_ROWS[s][p]
        return dirs.at[blk, pl.ds(r0, rn), :]

    def owner(p, m):
        return flip(me, frame_mask(p, m))

    def hi_bit(m):
        return 4 if m & 4 else (2 if m & 2 else 1)

    def landing(s, p, m, core_of=0):
        if s == 1 and m == 7:
            r0, rn = AG_ROWS[s][p]
            return late.at[core_of, pl.ds(r0, rn), :]
        dev = owner(p, m)
        return rows_of(s, p, 2 * (other_core(dev) if core_of else dev) + s)

    def ag_copy(s, p, m):
        top = hi_bit(m)
        held = m - top
        r0, rn = AG_ROWS[s][p]
        blk = 2 * owner(p, held) + s
        src = dstage.at[s, pl.ds(r0, rn), :] if held == 0 else rows_of(s, p, blk)
        dst = landing(s, p, m) if m == 7 and s == 1 else rows_of(s, p, blk)
        return pltpu.make_async_remote_copy(
            src_ref=src, dst_ref=dst, send_sem=ag_s.at[s], recv_sem=ag_r.at[s, m - 1],
            device_id=(owner(p, top),), device_id_type=MESH)

    def tile_like(s, m, core_of):
        return late.at[core_of] if m == 7 and s == 1 else dirs.at[0]

    def dd_copy(s, p, m):
        ref = landing(s, p, m)
        return pltpu.make_async_remote_copy(
            src_ref=ref, dst_ref=landing(s, p, m, 1) if m == 7 and s == 1 else ref,
            send_sem=dd_s.at[s], recv_sem=dd_r.at[s, m - 1], device_id=(mate,), device_id_type=MESH)

    def dd_wait(s, ms):
        for m in ms:
            wait_all(tile_like(s, m, 1), dd_s.at[s], dd_r.at[s, m - 1]).wait_recv()

    def own_local(s):
        return pltpu.make_async_copy(dstage.at[s], dirs.at[2 * me + s], own_sem.at[s])

    def own_mate(s, recv=False):
        blk = 2 * (mate if recv else me) + s
        return pltpu.make_async_remote_copy(
            src_ref=dstage.at[s], dst_ref=dirs.at[blk], send_sem=do_s.at[s], recv_sem=do_r.at[s],
            device_id=(mate,), device_id_type=MESH)

    def ag_start(s):
        for m in (1, 2, 4):
            for p in range(3):
                ag_copy(s, p, m).start()
        own_mate(s).start()
        own_local(s).start()

    def ag_take(s, ms):
        for m in ms:
            wait_all(tile_like(s, m, 0), ag_s.at[s], ag_r.at[s, m - 1]).wait_recv()
            for nxt in (2, 4):
                if nxt > m:
                    for p in range(3):
                        ag_copy(s, p, m | nxt).start()
            for p in range(3):
                dd_copy(s, p, m).start()

    for j in range(4):
        rs_take(0, j, (4 + j,) if j < 2 else ())
    prep_roots(0)
    prep_roots(1)
    for j in range(4):
        rs_take(1, j)
    rs_take(0, 4, (6,))
    for j in (4, 5):
        for p in range(3):
            rs_copy(1, p, j).start()
    for j in (5, 6):
        rs_take(0, j)
    for n in range(4):
        state_wait(n)
    block_math(0)
    ag_start(0)
    rs_take(1, 4, (6,))
    stats(0)
    rs_take(1, 5)
    ag_take(0, (1, 2))
    rs_take(1, 6)
    block_math(1)
    ag_start(1)

    wait_all(w2v.at[pl.ds(0, 7)], rs_s.at[0], rs_r.at[0, 0]).wait_send()
    w_copies = [
        pltpu.make_async_copy(w1.at[pl.ds(0, B)], w1a, w_sem.at[0]),
        pltpu.make_async_copy(w1.at[pl.ds(B, B)], w1b, w_sem.at[1])]
    w_copies += [pltpu.make_async_copy(w2.at[pl.ds(n * B, B)], w2v.at[n], w_sem.at[2 + n]) for n in range(8)]
    for cp in w_copies:
        cp.start()
    square_out().start()
    ag_take(0, (3,))
    stats(1)

    def ring(slot):
        return ybuf.at[lax.div(slot, 2), :, span(lax.rem(slot, 2), B)]

    def d_load(blk, slot):
        return pltpu.make_async_copy(dirs.at[blk], ring(slot), db_sem.at[slot])

    def apply_rows(out_ref, c, src):
        cols = span(c, B)

        def rows(rr, _):
            w = out_ref[rr, cols]
            out_ref[rr, cols] = w - LEARN_RATE * (src[rr, :].astype(F32) + WEIGHT_DECAY * w)

        sweep(rows)

    def apply_block(blk, src):
        @pl.when(blk < 8)
        def _():
            apply_rows(w1a, blk, src)

        @pl.when((blk >= 8) & (blk < N_DEV))
        def _():
            apply_rows(w1b, blk - 8, src)

        @pl.when(blk >= N_DEV)
        def _():
            apply_rows(w2v.at[lax.div(blk - N_DEV, 2)], lax.rem(blk, 2), src)

    def apply_range(blk_of, last, early=None, ready=None):
        def load(t):
            t = jnp.int32(t)
            return d_load(blk_of(t), t)

        for t in range(last):
            if t == early:
                ready()
            load(t).start()

        def step(t, _):
            load(t).wait()
            apply_block(blk_of(t), ring(t))
            return 0

        lax.fori_loop(0, last, step, 0)

    def landed(dev, s, t):
        return 2 * move(dev, bits_of(jnp.int32(LANDING[0]), LANDING, t)) + s

    def between(dev):
        return lambda t: landed(dev, jnp.where(t == 0, 0, 1), jnp.where(t == 0, 7, t - 1))

    def sent(s):
        wait_all(dirs.at[pl.ds(0, 7)], ag_s.at[s], ag_r.at[s, 0]).wait_send()
        wait_all(dirs.at[pl.ds(0, 7)], dd_s.at[s], dd_r.at[s, 0]).wait_send()

    ag_take(1, (1, 2))
    for cp in w_copies:
        cp.wait()
    for s in range(2):
        own_local(s).wait()
        own_mate(s).wait_send()
        own_mate(s, True).wait_recv()
    ag_take(0, (4, 5, 6))
    apply_range(lambda t: landed(me, 0, t), 7)
    dd_wait(0, range(1, 7))
    apply_range(lambda t: landed(mate, 0, t), 7)
    ag_take(0, (7,))
    ag_take(1, (4,))
    apply_range(between(me), 5)
    dd_wait(0, (7,))
    dd_wait(1, (1, 2, 4))
    apply_range(between(mate), 5)
    ag_take(1, (3,))
    sent(0)
    square_out().wait()
    ag_take(1, (5, 6))
    apply_range(lambda t: landed(jnp.where(t < 3, me, mate), 1, 4 + lax.rem(t, 3)), 6, 3, lambda: dd_wait(1, (3, 5, 6)))
    ag_take(1, (7,))
    apply_block(landed(me, 1, 7), late.at[0])
    dd_wait(1, (7,))
    apply_block(landed(mate, 1, 7), late.at[1])
    sent(1)


def write_out(w1a, w1b, w2v, v_l, v_r, v_m, kept, ow1, ow2, o_l, o_r, o_a, o_m, v_a, in_sem, sem):
    load = pltpu.make_async_copy(kept.at[0], v_a, in_sem.at[0])
    pairs = [(v_a, o_a), (v_l, o_l), (v_r, o_r), (v_m, o_m), (w1a, ow1.at[pl.ds(0, B)]), (w1b, ow1.at[pl.ds(B, B)])]
    pairs += [(w2v.at[n], ow2.at[pl.ds(n * B, B)]) for n in range(8)]
    stores = [pltpu.make_async_copy(src, dst, sem.at[n]) for n, (src, dst) in enumerate(pairs)]
    for cp in [load] + stores[1:]:
        cp.start()
    load.wait()
    for cp in stores[:1]:
        cp.start()
    for cp in stores:
        cp.wait()


def solution(mesh):
    def per_device(x_in, dy_mid, x_mid, dy_out, w_fc1, w_fc2, stat_left, stat_right, root_left, root_right, graft_sq, momentum):
        vmem = pl.BlockSpec(memory_space=pltpu.VMEM)
        hbm = pl.BlockSpec(memory_space=pltpu.HBM)
        dma = pltpu.SemaphoreType.DMA
        half = pltpu.VMEM((B, w_fc1.shape[1]), F32)
        kept = pltpu.HBM((N_DEV,) + stat_left.shape, F32)
        state = held = pltpu.VMEM(stat_left.shape, F32)
        tiles = pltpu.VMEM((2, B, B), BF16)
        parts = dma((2, 7))
        pair = dma((2,))
        *done, _ = pl.pallas_call(
            body,
            out_shape=(half, half, pltpu.VMEM((8, B, B2), F32), state, state, state, kept, pltpu.HBM((2 * N_DEV, B, B), BF16)),
            in_specs=[hbm] * 12,
            out_specs=(vmem,) * 6 + (hbm,) * 2,
            scratch_shapes=[
                pltpu.VMEM((DEPTH, B, B), BF16), pltpu.VMEM((DEPTH, B, B2), BF16), pltpu.VMEM((2, B, B2), F32), tiles, tiles, held,
                dma((2, DEPTH)), dma((4,)), dma((1,)), dma((2, 2)), dma((10,)), pair, dma((RING,)), dma((1,)), dma((2, 2)),
                dma((1,)), parts, pair, parts, pair, parts, pair, pair],
            compiler_params=pltpu.CompilerParams(collective_id=0, has_side_effects=True, vmem_limit_bytes=VMEM_GRANT),
            name='shampoo_step',
        )(x_in, dy_mid, x_mid, dy_out, w_fc1, w_fc2, stat_left, stat_right, root_left, root_right, graft_sq, momentum)
        like = (w_fc1, w_fc2, stat_left, stat_right, graft_sq, momentum)
        return pl.pallas_call(
            write_out,
            out_shape=tuple(jax.ShapeDtypeStruct(v.shape, F32) for v in like),
            in_specs=[vmem] * 6 + [hbm],
            out_specs=(hbm,) * 6,
            scratch_shapes=[held, dma((1,)), dma((14,))],
            compiler_params=pltpu.CompilerParams(vmem_limit_bytes=VMEM_GRANT),
            name='write_out',
        )(*done)

    row_spec = P('dp', None)
    rep_spec = P(None, None)
    tile_spec = P('dp', None, None)
    in_specs = (row_spec, row_spec, row_spec, row_spec, rep_spec, rep_spec, tile_spec, tile_spec, tile_spec, tile_spec, tile_spec, tile_spec)
    out_specs = (rep_spec, rep_spec, tile_spec, tile_spec, tile_spec, tile_spec)
    return jax.shard_map(per_device, mesh=mesh, in_specs=in_specs, out_specs=out_specs, check_vma=False)
```

```python
import functools

import jax
import jax.numpy as jnp
from jax import lax
from jax.experimental import pallas as pl
from jax.experimental.pallas import tpu as pltpu
from jax.sharding import PartitionSpec as P

STEP = 10
STAT_DECAY = 0.999
MOM_DECAY = 0.9
GRAFT_EPS = 1e-8
LEARN_RATE = 0.01
WEIGHT_DECAY = 1e-4
BIAS_CORR = 1.0 - STAT_DECAY ** STEP

MESH = pl.DeviceIdType.MESH
B = 512
B2 = 2 * B
CH = 32
HALF = B // 2
DEPTH = 4
RING = 8
VMEM_GRANT = 27 << 19
N_DEV = 16
ORDER = (7, 3, 5, 6, 1, 2, 4, 0)
LANDING = (0, 1, 2, 4, 3, 5, 6, 7)
AXES = ((1, 2, 4), (2, 4, 1), (4, 1, 2))
RS_ROWS = (((0, 176), (176, 168), (344, 168)), ((0, 168), (168, 176), (344, 168)))
AG_ROWS = (((0, 176), (176, 176), (352, 160)), ((0, 176), (176, 160), (336, 176)))
F32 = jnp.float32
BF16 = jnp.bfloat16


def flip(dev, mask):
    out = dev
    for bit in (1, 2, 4):
        if mask & bit:
            width = 2 * bit
            out = out + width - 2 * width * lax.rem(lax.div(dev, width), 2)
    return out


def other_core(dev):
    return dev + 1 - 2 * lax.rem(dev, 2)


def frame_mask(p, m):
    return sum(AXES[p][i] for i in range(3) if m & (1 << i))


def split(v):
    hi = v.astype(BF16)
    return hi, (v - hi.astype(F32)).astype(BF16)


def dot(a, b, ca, cb):
    return lax.dot_general(a, b, (((ca,), (cb,)), ((), ())), preferred_element_type=F32)


def dot_tn(a, b):
    return dot(a, b, 0, 0)


def dot3(a_hi, a_lo, b_hi, b_lo, ca, cb):
    return dot(a_hi, b_hi, ca, cb) + (dot(a_hi, b_lo, ca, cb) + dot(a_lo, b_hi, ca, cb))


def span(t, size):
    return pl.ds(pl.multiple_of(t * size, size), size)


def sweep(fn, init=None):
    def step(t, carry):
        out = fn(span(t, CH), carry)
        return carry if out is None else out

    return lax.fori_loop(0, B // CH, step, jnp.int32(0) if init is None else init)


def bits_of(rel, table, t):
    for n, value in enumerate(table):
        if n:
            rel = jnp.where(t == n, value, rel)
    return rel


def move(dev, rel):
    out = lax.rem(dev, 2)
    for bit in (1, 2, 4):
        out = out + 2 * bit * lax.rem(lax.div(dev, 2 * bit) + lax.div(rel, bit), 2)
    return out


def body(x_in, dy_mid, x_mid, dy_out, w1, w2, st_l, st_r, rt_l, rt_r, gsq, mom,
         w1a, w1b, w2v, v_l, v_r, v_a, v_m, dirs,
         xbuf, ybuf, res, dstage, late,
         op_sem, st_sem, rt_sem, w_sem, own_sem, db_sem, d2d_s, d2d_r, rs_s, rs_r, ag_s, ag_r, dd_s, dd_r, do_s, do_r):
    me = lax.axis_index('dp')
    core = lax.rem(me, 2)
    mate = other_core(me)

    barrier = pltpu.get_barrier_semaphore()
    for nb in (mate, flip(me, 1), flip(me, 2), flip(me, 4)):
        pl.semaphore_signal(barrier, inc=1, device_id=(nb,), device_id_type=MESH)

    def op_start(q):
        h = lax.rem(q, DEPTH)
        side = lax.div(q, DEPTH)
        dest = move(me, bits_of(jnp.int32(ORDER[0]), ORDER, lax.div(side, 2)))
        kd = jnp.where(lax.rem(side, 2) == 0, other_core(dest), dest)
        rows = span(h, B)

        @pl.when(dest < N_DEV // 2)
        def _():
            pltpu.make_async_copy(x_in.at[rows, span(lax.div(kd, 4), B)], xbuf.at[h], op_sem.at[0, h]).start()
            pltpu.make_async_copy(dy_mid.at[rows, span(lax.rem(kd, 4), B2)], ybuf.at[h], op_sem.at[1, h]).start()

        @pl.when(dest >= N_DEV // 2)
        def _():
            pltpu.make_async_copy(x_mid.at[rows, span(kd - N_DEV // 2, B)], xbuf.at[h], op_sem.at[0, h]).start()
            pltpu.make_async_copy(dy_out.at[rows, :], ybuf.at[h], op_sem.at[1, h]).start()

    def op_wait(h):
        pltpu.make_async_copy(x_in.at[pl.ds(0, B), pl.ds(0, B)], xbuf.at[h], op_sem.at[0, h]).wait()
        pltpu.make_async_copy(dy_mid.at[pl.ds(0, B), pl.ds(0, B2)], ybuf.at[h], op_sem.at[1, h]).wait()

    for q in range(DEPTH):
        op_start(jnp.int32(q))
    states = ((st_l, v_l), (st_r, v_r), (gsq, v_a), (mom, v_m))
    def acc_at(i, r0, rn, c0, cn):
        return (w1a, w1b)[i // 4].at[pl.ds(r0, rn), pl.ds((i % 4) * B2 + c0, cn)]

    def acc_of(rel, s, p):
        r0, rn = RS_ROWS[s][p]
        return acc_at(ORDER.index(rel), r0, rn, s * B, B)

    def got(s, p, j):
        r0, rn = RS_ROWS[s][p]
        return w2v.at[j, pl.ds(r0, rn), pl.ds(s * B, B)]

    def rs_rel(p, j):
        a1, a2, a3 = AXES[p]
        return (a2 | a3, a2, a3, 0, a3, 0, 0)[j]

    def rs_copy(s, p, j):
        axis = AXES[p][0 if j < 4 else (1 if j < 6 else 2)]
        return pltpu.make_async_remote_copy(
            src_ref=acc_of(rs_rel(p, j) | axis, s, p), dst_ref=got(s, p, j),
            send_sem=rs_s.at[0], recv_sem=rs_r.at[s, j],
            device_id=(flip(me, axis),), device_id_type=MESH)

    def wait_all(ref, send_sem, recv_sem):
        return pltpu.make_async_remote_copy(
            src_ref=ref, dst_ref=ref, send_sem=send_sem, recv_sem=recv_sem, device_id=(mate,), device_id_type=MESH)

    def rs_take(s, j, then=()):
        wait_all(w2v.at[j, :, pl.ds(s * B, B)], rs_s.at[0], rs_r.at[s, j]).wait_recv()
        for p in range(3):
            ref = acc_of(rs_rel(p, j), s, p)
            ref[...] += got(s, p, j)[...]
            for nxt in then:
                rs_copy(s, p, nxt).start()

    def d2d_copy(i, s, half):
        return pltpu.make_async_remote_copy(
            src_ref=res.at[0, :, pl.ds(s * B, B)], dst_ref=half.at[:, span(lax.rem(i, 4) * 2 + s, B)],
            send_sem=d2d_s.at[0], recv_sem=d2d_r.at[s, lax.rem(i, 2)], device_id=(mate,), device_id_type=MESH)

    def on_half(i, fn):
        @pl.when(i < 4)
        def _():
            fn(w1a)

        @pl.when(i >= 4)
        def _():
            fn(w1b)

    def add_mine(i, s, half):
        d2d_copy(i, s, half).wait_recv()
        cols = span(lax.rem(i, 4) * 2 + s, B)

        def add_rows(rr, _):
            half[rr, cols] += res[1, rr, pl.ds(s * B, B)]

        sweep(add_rows)

    def send_on(ii, s):
        for p in range(3):
            for jj in range(4):
                if (rs_rel(p, jj) | AXES[p][0]) == ORDER[ii]:
                    rs_copy(s, p, jj).start()

    for j in range(2):
        for s in range(2):
            cols = pl.ds(s * B, B)
            for h in range(DEPTH):
                if s == 0:
                    op_wait(h)
                    prod = dot_tn(xbuf[h], ybuf[h, :, cols])
                else:
                    prod = dot_tn(xbuf[h], ybuf[h, :, cols])
                    if j == 0 or h < DEPTH - 1:
                        op_start(jnp.int32((j + 1) * DEPTH + h))
                if h:
                    res[j, :, cols] += prod
                else:
                    res[j, :, cols] = prod
            if j == 0:
                if s == 0:
                    pl.semaphore_wait(barrier, 4)
                d2d_copy(jnp.int32(0), s, w1a).start()
            else:
                add_mine(jnp.int32(0), s, w1a)
                send_on(0, s)

    def compute_step(i, _):
        wait_all(res.at[0], d2d_s.at[0], d2d_r.at[0, 0]).wait_send()

        def side(j, _):
            for h in range(DEPTH):
                ahead = (i * 2 + j) * DEPTH + h + DEPTH - 1

                @pl.when(ahead < 2 * 8 * DEPTH)
                def _(ahead=ahead):
                    op_start(ahead)
                op_wait(h)
                if h:
                    res[j] += dot_tn(xbuf[h], ybuf[h])
                else:
                    res[j] = dot_tn(xbuf[h], ybuf[h])

            @pl.when(j == 0)
            def _():
                on_half(i, lambda half: [d2d_copy(i, s, half).start() for s in range(2)])
            return 0

        lax.fori_loop(0, 2, side, 0)
        for s in range(2):
            on_half(i, lambda half, s=s: add_mine(i, s, half))
            for ii in range(1, 7):
                @pl.when(i == ii)
                def _(ii=ii, s=s):
                    send_on(ii, s)
        return 0

    lax.fori_loop(1, 8, compute_step, 0)
    wait_all(res.at[0], d2d_s.at[0], d2d_r.at[0, 0]).wait_send()

    for n, (src, dst) in enumerate(states):
        pltpu.make_async_copy(src, dst, st_sem.at[n]).start()

    def root_half(s, side):
        return res.at[s, :, pl.ds(side * B, B)]

    for s in range(2):
        for side, src in enumerate((rt_l, rt_r)):
            pltpu.make_async_copy(src.at[s], root_half(s, side), rt_sem.at[s, side]).start()

    def root_hi(s, side):
        return ybuf.at[s, :, pl.ds(side * B, B)]

    def root_lo(s, side):
        return ybuf.at[2 + s, :, pl.ds(side * B, B)]

    def g_hi(s):
        return xbuf.at[s]

    def g_lo(s):
        return xbuf.at[2 + s]

    def prep_roots(s):
        for side, src in enumerate((rt_l, rt_r)):
            pltpu.make_async_copy(src.at[s], root_half(s, side), rt_sem.at[s, side]).wait()

        def rows(rr, _):
            for side in range(2):
                root_hi(s, side)[rr, :], root_lo(s, side)[rr, :] = split(root_half(s, side)[rr, :])

        sweep(rows)

    def state_wait(n):
        pltpu.make_async_copy(states[n][0], states[n][1], st_sem.at[n]).wait()

    first_cols = pl.ds(0, B)

    def block_math(s):
        gref = acc_at(ORDER.index(0), 0, B, s * B, B)
        zero = jnp.zeros((8, B), F32)

        def first(rr, tot):
            g = gref[rr, :] * (1.0 / N_DEV)
            g_hi(s)[rr, :], g_lo(s)[rr, :] = split(g)
            sq = STAT_DECAY * v_a[s, rr, :] + (1.0 - STAT_DECAY) * g * g
            v_a[s, rr, :] = sq
            h = g / (jnp.sqrt(sq / BIAS_CORR) + GRAFT_EPS)
            return tot + jnp.sum((h * h).reshape(-1, 8, B), axis=0)

        h_sum = sweep(first, zero)

        def left(t, _):
            rr = span(t, HALF)
            v = dot3(root_hi(s, 0)[rr, :], root_lo(s, 0)[rr, :], g_hi(s)[...], g_lo(s)[...], 1, 0)
            g_hi(1 - s)[rr, :], g_lo(1 - s)[rr, :] = split(v)
            return 0

        lax.fori_loop(0, 2, left, 0)

        def right(t, tot):
            rr = span(t, HALF)
            v = dot3(g_hi(1 - s)[rr, :], g_lo(1 - s)[rr, :], root_hi(s, 1)[...], root_lo(s, 1)[...], 1, 0)
            res[0, rr, first_cols] = v
            return tot + jnp.sum((v * v).reshape(-1, 8, B), axis=0)

        p_sum = lax.fori_loop(0, 2, right, zero)
        ratio = jnp.sqrt(jnp.sum(h_sum, keepdims=True)) / jnp.sqrt(jnp.sum(p_sum, keepdims=True))

        def last(rr, _):
            m = MOM_DECAY * v_m[s, rr, :] + res[0, rr, first_cols] * ratio
            v_m[s, rr, :] = m
            dstage[s, rr, :] = m.astype(BF16)

        sweep(last)

    def stats(s):
        hi, lo = g_hi(s), g_lo(s)
        for t in range(2):
            rr = pl.ds(t * HALF, HALF)
            left = dot3(hi[rr, :], lo[rr, :], hi[...], lo[...], 1, 1)
            v_l[s, rr, :] = STAT_DECAY * v_l[s, rr, :] + (1.0 - STAT_DECAY) * left
            right = dot3(hi[:, rr], lo[:, rr], hi[...], lo[...], 0, 0)
            v_r[s, rr, :] = STAT_DECAY * v_r[s, rr, :] + (1.0 - STAT_DECAY) * right

    def rows_of(s, p, blk):
        r0, rn = AG_ROWS[s][p]
        return dirs.at[blk, pl.ds(r0, rn), :]

    def owner(p, m):
        return flip(me, frame_mask(p, m))

    def hi_bit(m):
        return 4 if m & 4 else (2 if m & 2 else 1)

    def landing(s, p, m, core_of=0):
        if s == 1 and m == 7:
            r0, rn = AG_ROWS[s][p]
            return late.at[core_of, pl.ds(r0, rn), :]
        dev = owner(p, m)
        return rows_of(s, p, 2 * (other_core(dev) if core_of else dev) + s)

    def ag_copy(s, p, m):
        top = hi_bit(m)
        held = m - top
        r0, rn = AG_ROWS[s][p]
        blk = 2 * owner(p, held) + s
        src = dstage.at[s, pl.ds(r0, rn), :] if held == 0 else rows_of(s, p, blk)
        dst = landing(s, p, m) if m == 7 and s == 1 else rows_of(s, p, blk)
        return pltpu.make_async_remote_copy(
            src_ref=src, dst_ref=dst, send_sem=ag_s.at[s], recv_sem=ag_r.at[s, m - 1],
            device_id=(owner(p, top),), device_id_type=MESH)

    def tile_like(s, m, core_of):
        return late.at[core_of] if m == 7 and s == 1 else dirs.at[0]

    def dd_copy(s, p, m):
        ref = landing(s, p, m)
        return pltpu.make_async_remote_copy(
            src_ref=ref, dst_ref=landing(s, p, m, 1) if m == 7 and s == 1 else ref,
            send_sem=dd_s.at[s], recv_sem=dd_r.at[s, m - 1], device_id=(mate,), device_id_type=MESH)

    def dd_wait(s, ms):
        for m in ms:
            wait_all(tile_like(s, m, 1), dd_s.at[s], dd_r.at[s, m - 1]).wait_recv()

    def own_local(s):
        return pltpu.make_async_copy(dstage.at[s], dirs.at[2 * me + s], own_sem.at[s])

    def own_mate(s, recv=False):
        blk = 2 * (mate if recv else me) + s
        return pltpu.make_async_remote_copy(
            src_ref=dstage.at[s], dst_ref=dirs.at[blk], send_sem=do_s.at[s], recv_sem=do_r.at[s],
            device_id=(mate,), device_id_type=MESH)

    def ag_start(s):
        for m in (1, 2, 4):
            for p in range(3):
                ag_copy(s, p, m).start()
        own_mate(s).start()
        own_local(s).start()

    def ag_take(s, ms):
        for m in ms:
            wait_all(tile_like(s, m, 0), ag_s.at[s], ag_r.at[s, m - 1]).wait_recv()
            for nxt in (2, 4):
                if nxt > m:
                    for p in range(3):
                        ag_copy(s, p, m | nxt).start()
            for p in range(3):
                dd_copy(s, p, m).start()

    for j in range(4):
        rs_take(0, j, (4 + j,) if j < 2 else ())
    prep_roots(0)
    prep_roots(1)
    for j in range(4):
        rs_take(1, j)
    rs_take(0, 4, (6,))
    for j in (4, 5):
        for p in range(3):
            rs_copy(1, p, j).start()
    for j in (5, 6):
        rs_take(0, j)
    for n in range(4):
        state_wait(n)
    block_math(0)
    ag_start(0)
    rs_take(1, 4, (6,))
    stats(0)
    rs_take(1, 5)
    ag_take(0, (1, 2))
    rs_take(1, 6)
    block_math(1)
    ag_start(1)

    wait_all(w2v.at[pl.ds(0, 7)], rs_s.at[0], rs_r.at[0, 0]).wait_send()
    w_copies = [
        pltpu.make_async_copy(w1.at[pl.ds(0, B)], w1a, w_sem.at[0]),
        pltpu.make_async_copy(w1.at[pl.ds(B, B)], w1b, w_sem.at[1])]
    w_copies += [pltpu.make_async_copy(w2.at[pl.ds(n * B, B)], w2v.at[n], w_sem.at[2 + n]) for n in range(8)]
    for cp in w_copies:
        cp.start()
    ag_take(0, (3,))
    stats(1)

    def ring(slot):
        return ybuf.at[lax.div(slot, 2), :, span(lax.rem(slot, 2), B)]

    def d_load(blk, slot):
        return pltpu.make_async_copy(dirs.at[blk], ring(slot), db_sem.at[slot])

    def apply_rows(out_ref, c, src):
        cols = span(c, B)

        def rows(rr, _):
            w = out_ref[rr, cols]
            out_ref[rr, cols] = w - LEARN_RATE * (src[rr, :].astype(F32) + WEIGHT_DECAY * w)

        sweep(rows)

    def apply_block(blk, src):
        @pl.when(blk < 8)
        def _():
            apply_rows(w1a, blk, src)

        @pl.when((blk >= 8) & (blk < N_DEV))
        def _():
            apply_rows(w1b, blk - 8, src)

        @pl.when(blk >= N_DEV)
        def _():
            apply_rows(w2v.at[lax.div(blk - N_DEV, 2)], lax.rem(blk, 2), src)

    def apply_range(blk_of, last, early=None, ready=None):
        def load(t):
            t = jnp.int32(t)
            return d_load(blk_of(t), t)

        for t in range(last):
            if t == early:
                ready()
            load(t).start()

        def step(t, _):
            load(t).wait()
            apply_block(blk_of(t), ring(t))
            return 0

        lax.fori_loop(0, last, step, 0)

    def landed(dev, s, t):
        return 2 * move(dev, bits_of(jnp.int32(LANDING[0]), LANDING, t)) + s

    def between(dev):
        return lambda t: landed(dev, jnp.where(t == 0, 0, 1), jnp.where(t == 0, 7, t - 1))

    def sent(s):
        wait_all(dirs.at[pl.ds(0, 7)], ag_s.at[s], ag_r.at[s, 0]).wait_send()
        wait_all(dirs.at[pl.ds(0, 7)], dd_s.at[s], dd_r.at[s, 0]).wait_send()

    ag_take(1, (1, 2))
    for cp in w_copies:
        cp.wait()
    for s in range(2):
        own_local(s).wait()
        own_mate(s).wait_send()
        own_mate(s, True).wait_recv()
    ag_take(0, (4, 5, 6))
    apply_range(lambda t: landed(me, 0, t), 7)
    dd_wait(0, range(1, 7))
    apply_range(lambda t: landed(mate, 0, t), 7)
    ag_take(0, (7,))
    ag_take(1, (4,))
    apply_range(between(me), 5)
    dd_wait(0, (7,))
    dd_wait(1, (1, 2, 4))
    apply_range(between(mate), 5)
    ag_take(1, (3,))
    sent(0)
    ag_take(1, (5, 6))
    apply_range(lambda t: landed(jnp.where(t < 3, me, mate), 1, 4 + lax.rem(t, 3)), 6, 3, lambda: dd_wait(1, (3, 5, 6)))
    ag_take(1, (7,))
    apply_block(landed(me, 1, 7), late.at[0])
    dd_wait(1, (7,))
    apply_block(landed(mate, 1, 7), late.at[1])
    sent(1)


def write_out(w1a, w1b, w2v, v_l, v_r, v_a, v_m, ow1, ow2, o_l, o_r, o_a, o_m, sem):
    pairs = [(w1a, ow1.at[pl.ds(0, B)]), (w1b, ow1.at[pl.ds(B, B)]), (v_l, o_l), (v_r, o_r), (v_a, o_a), (v_m, o_m)]
    pairs += [(w2v.at[n], ow2.at[pl.ds(n * B, B)]) for n in range(8)]
    stores = [pltpu.make_async_copy(src, dst, sem.at[n]) for n, (src, dst) in enumerate(pairs)]
    for cp in stores:
        cp.start()
    for cp in stores:
        cp.wait()


def solution(mesh):
    def per_device(x_in, dy_mid, x_mid, dy_out, w_fc1, w_fc2, stat_left, stat_right, root_left, root_right, graft_sq, momentum):
        vmem = pl.BlockSpec(memory_space=pltpu.VMEM)
        hbm = pl.BlockSpec(memory_space=pltpu.HBM)
        dma = pltpu.SemaphoreType.DMA
        half = pltpu.VMEM((B, w_fc1.shape[1]), F32)
        state = pltpu.VMEM(stat_left.shape, F32)
        tiles = pltpu.VMEM((2, B, B), BF16)
        parts = dma((2, 7))
        pair = dma((2,))
        *done, _ = pl.pallas_call(
            body,
            out_shape=(half, half, pltpu.VMEM((8, B, B2), F32), state, state, state, state, pltpu.HBM((2 * N_DEV, B, B), BF16)),
            in_specs=[hbm] * 12,
            out_specs=(vmem,) * 7 + (hbm,),
            scratch_shapes=[
                pltpu.VMEM((DEPTH, B, B), BF16), pltpu.VMEM((DEPTH, B, B2), BF16), pltpu.VMEM((2, B, B2), F32), tiles, tiles,
                dma((2, DEPTH)), dma((4,)), dma((2, 2)), dma((10,)), pair, dma((RING,)), dma((1,)), dma((2, 2)),
                dma((1,)), parts, pair, parts, pair, parts, pair, pair],
            compiler_params=pltpu.CompilerParams(collective_id=0, has_side_effects=True, vmem_limit_bytes=VMEM_GRANT),
            name='shampoo_step',
        )(x_in, dy_mid, x_mid, dy_out, w_fc1, w_fc2, stat_left, stat_right, root_left, root_right, graft_sq, momentum)
        like = (w_fc1, w_fc2, stat_left, stat_right, graft_sq, momentum)
        return pl.pallas_call(
            write_out,
            out_shape=tuple(jax.ShapeDtypeStruct(v.shape, F32) for v in like),
            in_specs=[vmem] * 7,
            out_specs=(hbm,) * 6,
            scratch_shapes=[dma((14,))],
            compiler_params=pltpu.CompilerParams(vmem_limit_bytes=VMEM_GRANT),
            name='write_out',
        )(*done)

    row_spec = P('dp', None)
    rep_spec = P(None, None)
    tile_spec = P('dp', None, None)
    in_specs = (row_spec, row_spec, row_spec, row_spec, rep_spec, rep_spec, tile_spec, tile_spec, tile_spec, tile_spec, tile_spec, tile_spec)
    out_specs = (rep_spec, rep_spec, tile_spec, tile_spec, tile_spec, tile_spec)
    return jax.shard_map(per_device, mesh=mesh, in_specs=in_specs, out_specs=out_specs, check_vma=False)
```

```python
import functools

import jax
import jax.numpy as jnp
from jax import lax
from jax.experimental import pallas as pl
from jax.experimental.pallas import tpu as pltpu
from jax.sharding import PartitionSpec as P

STEP = 10
STAT_DECAY = 0.999
MOM_DECAY = 0.9
GRAFT_EPS = 1e-8
LEARN_RATE = 0.01
WEIGHT_DECAY = 1e-4
BIAS_CORR = 1.0 - STAT_DECAY ** STEP

MESH = pl.DeviceIdType.MESH
B = 512
B2 = 2 * B
CH = 32
HALF = B // 2
DEPTH = 4
RING = 8
VMEM_GRANT = 27 << 19
N_DEV = 16
ORDER = (7, 3, 5, 6, 1, 2, 4, 0)
LANDING = (0, 1, 2, 4, 3, 5, 6, 7)
AXES = ((1, 2, 4), (2, 4, 1), (4, 1, 2))
RS_ROWS = (((0, 176), (176, 168), (344, 168)), ((0, 168), (168, 176), (344, 168)))
AG_ROWS = (((0, 176), (176, 176), (352, 160)), ((0, 176), (176, 160), (336, 176)))
F32 = jnp.float32
BF16 = jnp.bfloat16


def flip(dev, mask):
    out = dev
    for bit in (1, 2, 4):
        if mask & bit:
            width = 2 * bit
            out = out + width - 2 * width * lax.rem(lax.div(dev, width), 2)
    return out


def other_core(dev):
    return dev + 1 - 2 * lax.rem(dev, 2)


def frame_mask(p, m):
    return sum(AXES[p][i] for i in range(3) if m & (1 << i))


def split(v):
    hi = v.astype(BF16)
    return hi, (v - hi.astype(F32)).astype(BF16)


def dot(a, b, ca, cb):
    return lax.dot_general(a, b, (((ca,), (cb,)), ((), ())), preferred_element_type=F32)


def dot_tn(a, b):
    return dot(a, b, 0, 0)


def dot3(a_hi, a_lo, b_hi, b_lo, ca, cb):
    return dot(a_hi, b_hi, ca, cb) + (dot(a_hi, b_lo, ca, cb) + dot(a_lo, b_hi, ca, cb))


def span(t, size):
    return pl.ds(pl.multiple_of(t * size, size), size)


def sweep(fn, init=None):
    def step(t, carry):
        out = fn(span(t, CH), carry)
        return carry if out is None else out

    return lax.fori_loop(0, B // CH, step, jnp.int32(0) if init is None else init)


def bits_of(rel, table, t):
    for n, value in enumerate(table):
        if n:
            rel = jnp.where(t == n, value, rel)
    return rel


def move(dev, rel):
    out = lax.rem(dev, 2)
    for bit in (1, 2, 4):
        out = out + 2 * bit * lax.rem(lax.div(dev, 2 * bit) + lax.div(rel, bit), 2)
    return out


def body(x_in, dy_mid, x_mid, dy_out, w1, w2, st_l, st_r, rt_l, rt_r, gsq, mom,
         w1a, w1b, w2v, v_l, v_r, v_a, v_m, dirs,
         xbuf, ybuf, res, dstage, late,
         op_sem, st_sem, rt_sem, w_sem, own_sem, db_sem, d2d_s, d2d_r, rs_s, rs_r, ag_s, ag_r, dd_s, dd_r, do_s, do_r):
    me = lax.axis_index('dp')
    core = lax.rem(me, 2)
    mate = other_core(me)

    barrier = pltpu.get_barrier_semaphore()
    for nb in (mate, flip(me, 1), flip(me, 2), flip(me, 4)):
        pl.semaphore_signal(barrier, inc=1, device_id=(nb,), device_id_type=MESH)

    def op_start(q):
        h = lax.rem(q, DEPTH)
        side = lax.div(q, DEPTH)
        dest = move(me, bits_of(jnp.int32(ORDER[0]), ORDER, lax.div(side, 2)))
        kd = jnp.where(lax.rem(side, 2) == 0, other_core(dest), dest)
        rows = span(h, B)

        @pl.when(dest < N_DEV // 2)
        def _():
            pltpu.make_async_copy(x_in.at[rows, span(lax.div(kd, 4), B)], xbuf.at[h], op_sem.at[0, h]).start()
            pltpu.make_async_copy(dy_mid.at[rows, span(lax.rem(kd, 4), B2)], ybuf.at[h], op_sem.at[1, h]).start()

        @pl.when(dest >= N_DEV // 2)
        def _():
            pltpu.make_async_copy(x_mid.at[rows, span(kd - N_DEV // 2, B)], xbuf.at[h], op_sem.at[0, h]).start()
            pltpu.make_async_copy(dy_out.at[rows, :], ybuf.at[h], op_sem.at[1, h]).start()

    def op_wait(h):
        pltpu.make_async_copy(x_in.at[pl.ds(0, B), pl.ds(0, B)], xbuf.at[h], op_sem.at[0, h]).wait()
        pltpu.make_async_copy(dy_mid.at[pl.ds(0, B), pl.ds(0, B2)], ybuf.at[h], op_sem.at[1, h]).wait()

    passes = ((0, 0), (1, 0), (0, 1), (1, 1))

    def first_copies(n, h, fn):
        j, s = passes[n]
        kd = flip(me, ORDER[0]) if j else other_core(flip(me, ORDER[0]))
        rows = pl.ds(h * B, B)
        y_to = ybuf.at[h, :, pl.ds(0, B)]

        @pl.when(kd < N_DEV // 2)
        def _():
            fn(pltpu.make_async_copy(x_in.at[rows, span(lax.div(kd, 4), B)], xbuf.at[h], op_sem.at[0, h]))
            fn(pltpu.make_async_copy(dy_mid.at[rows, span(lax.rem(kd, 4) * 2 + s, B)], y_to, op_sem.at[1, h]))

        @pl.when(kd >= N_DEV // 2)
        def _():
            fn(pltpu.make_async_copy(x_mid.at[rows, span(kd - N_DEV // 2, B)], xbuf.at[h], op_sem.at[0, h]))
            fn(pltpu.make_async_copy(dy_out.at[rows, pl.ds(s * B, B)], y_to, op_sem.at[1, h]))

    for h in range(DEPTH):
        first_copies(0, h, lambda cp: cp.start())
    states = ((st_l, v_l), (st_r, v_r), (gsq, v_a), (mom, v_m))
    def acc_at(i, r0, rn, c0, cn):
        return (w1a, w1b)[i // 4].at[pl.ds(r0, rn), pl.ds((i % 4) * B2 + c0, cn)]

    def acc_of(rel, s, p):
        r0, rn = RS_ROWS[s][p]
        return acc_at(ORDER.index(rel), r0, rn, s * B, B)

    def got(s, p, j):
        r0, rn = RS_ROWS[s][p]
        return w2v.at[j, pl.ds(r0, rn), pl.ds(s * B, B)]

    def rs_rel(p, j):
        a1, a2, a3 = AXES[p]
        return (a2 | a3, a2, a3, 0, a3, 0, 0)[j]

    def rs_copy(s, p, j):
        axis = AXES[p][0 if j < 4 else (1 if j < 6 else 2)]
        return pltpu.make_async_remote_copy(
            src_ref=acc_of(rs_rel(p, j) | axis, s, p), dst_ref=got(s, p, j),
            send_sem=rs_s.at[0], recv_sem=rs_r.at[s, j],
            device_id=(flip(me, axis),), device_id_type=MESH)

    def wait_all(ref, send_sem, recv_sem):
        return pltpu.make_async_remote_copy(
            src_ref=ref, dst_ref=ref, send_sem=send_sem, recv_sem=recv_sem, device_id=(mate,), device_id_type=MESH)

    def rs_take(s, j, then=()):
        wait_all(w2v.at[j, :, pl.ds(s * B, B)], rs_s.at[0], rs_r.at[s, j]).wait_recv()
        for p in range(3):
            ref = acc_of(rs_rel(p, j), s, p)
            ref[...] += got(s, p, j)[...]
            for nxt in then:
                rs_copy(s, p, nxt).start()

    def d2d_copy(i, s, half):
        return pltpu.make_async_remote_copy(
            src_ref=res.at[0, :, pl.ds(s * B, B)], dst_ref=half.at[:, span(lax.rem(i, 4) * 2 + s, B)],
            send_sem=d2d_s.at[0], recv_sem=d2d_r.at[s, lax.rem(i, 2)], device_id=(mate,), device_id_type=MESH)

    def on_half(i, fn):
        @pl.when(i < 4)
        def _():
            fn(w1a)

        @pl.when(i >= 4)
        def _():
            fn(w1b)

    def add_mine(i, s, half):
        d2d_copy(i, s, half).wait_recv()
        cols = span(lax.rem(i, 4) * 2 + s, B)

        def add_rows(rr, _):
            half[rr, cols] += res[1, rr, pl.ds(s * B, B)]

        sweep(add_rows)

    def send_on(ii, s):
        for p in range(3):
            for jj in range(4):
                if (rs_rel(p, jj) | AXES[p][0]) == ORDER[ii]:
                    rs_copy(s, p, jj).start()

    for n, (j, s) in enumerate(passes):
        cols = pl.ds(s * B, B)
        for h in range(DEPTH):
            first_copies(n, h, lambda cp: cp.wait())
            prod = dot_tn(xbuf[h], ybuf[h, :, pl.ds(0, B)])
            if h:
                res[j, :, cols] += prod
            else:
                res[j, :, cols] = prod
            if n + 1 < len(passes):
                first_copies(n + 1, h, lambda cp: cp.start())
            elif h < DEPTH - 1:
                op_start(jnp.int32(2 * DEPTH + h))
        if n == 0:
            pl.semaphore_wait(barrier, 4)
        if j == 0:
            d2d_copy(jnp.int32(0), s, w1a).start()
        if n >= 2:
            add_mine(jnp.int32(0), n - 2, w1a)
            send_on(0, n - 2)

    def compute_step(i, _):
        wait_all(res.at[0], d2d_s.at[0], d2d_r.at[0, 0]).wait_send()

        def side(j, _):
            for h in range(DEPTH):
                ahead = (i * 2 + j) * DEPTH + h + DEPTH - 1

                @pl.when(ahead < 2 * 8 * DEPTH)
                def _(ahead=ahead):
                    op_start(ahead)
                op_wait(h)
                if h:
                    res[j] += dot_tn(xbuf[h], ybuf[h])
                else:
                    res[j] = dot_tn(xbuf[h], ybuf[h])

            @pl.when(j == 0)
            def _():
                on_half(i, lambda half: [d2d_copy(i, s, half).start() for s in range(2)])
            return 0

        lax.fori_loop(0, 2, side, 0)
        for s in range(2):
            on_half(i, lambda half, s=s: add_mine(i, s, half))
            for ii in range(1, 7):
                @pl.when(i == ii)
                def _(ii=ii, s=s):
                    send_on(ii, s)
        return 0

    lax.fori_loop(1, 8, compute_step, 0)
    wait_all(res.at[0], d2d_s.at[0], d2d_r.at[0, 0]).wait_send()

    for n, (src, dst) in enumerate(states):
        pltpu.make_async_copy(src, dst, st_sem.at[n]).start()

    def root_half(s, side):
        return res.at[s, :, pl.ds(side * B, B)]

    for s in range(2):
        for side, src in enumerate((rt_l, rt_r)):
            pltpu.make_async_copy(src.at[s], root_half(s, side), rt_sem.at[s, side]).start()

    def root_hi(s, side):
        return ybuf.at[s, :, pl.ds(side * B, B)]

    def root_lo(s, side):
        return ybuf.at[2 + s, :, pl.ds(side * B, B)]

    def g_hi(s):
        return xbuf.at[s]

    def g_lo(s):
        return xbuf.at[2 + s]

    def prep_roots(s):
        for side, src in enumerate((rt_l, rt_r)):
            pltpu.make_async_copy(src.at[s], root_half(s, side), rt_sem.at[s, side]).wait()

        def rows(rr, _):
            for side in range(2):
                root_hi(s, side)[rr, :], root_lo(s, side)[rr, :] = split(root_half(s, side)[rr, :])

        sweep(rows)

    def state_wait(n):
        pltpu.make_async_copy(states[n][0], states[n][1], st_sem.at[n]).wait()

    first_cols = pl.ds(0, B)

    def block_math(s):
        gref = acc_at(ORDER.index(0), 0, B, s * B, B)
        zero = jnp.zeros((8, B), F32)

        def first(rr, tot):
            g = gref[rr, :] * (1.0 / N_DEV)
            g_hi(s)[rr, :], g_lo(s)[rr, :] = split(g)
            sq = STAT_DECAY * v_a[s, rr, :] + (1.0 - STAT_DECAY) * g * g
            v_a[s, rr, :] = sq
            h = g / (jnp.sqrt(sq / BIAS_CORR) + GRAFT_EPS)
            return tot + jnp.sum((h * h).reshape(-1, 8, B), axis=0)

        h_sum = sweep(first, zero)

        def left(t, _):
            rr = span(t, HALF)
            v = dot3(root_hi(s, 0)[rr, :], root_lo(s, 0)[rr, :], g_hi(s)[...], g_lo(s)[...], 1, 0)
            g_hi(1 - s)[rr, :], g_lo(1 - s)[rr, :] = split(v)
            return 0

        lax.fori_loop(0, 2, left, 0)

        def right(t, tot):
            rr = span(t, HALF)
            v = dot3(g_hi(1 - s)[rr, :], g_lo(1 - s)[rr, :], root_hi(s, 1)[...], root_lo(s, 1)[...], 1, 0)
            res[0, rr, first_cols] = v
            return tot + jnp.sum((v * v).reshape(-1, 8, B), axis=0)

        p_sum = lax.fori_loop(0, 2, right, zero)
        ratio = jnp.sqrt(jnp.sum(h_sum, keepdims=True)) / jnp.sqrt(jnp.sum(p_sum, keepdims=True))

        def last(rr, _):
            m = MOM_DECAY * v_m[s, rr, :] + res[0, rr, first_cols] * ratio
            v_m[s, rr, :] = m
            dstage[s, rr, :] = m.astype(BF16)

        sweep(last)

    def stats(s):
        hi, lo = g_hi(s), g_lo(s)
        for t in range(2):
            rr = pl.ds(t * HALF, HALF)
            left = dot3(hi[rr, :], lo[rr, :], hi[...], lo[...], 1, 1)
            v_l[s, rr, :] = STAT_DECAY * v_l[s, rr, :] + (1.0 - STAT_DECAY) * left
            right = dot3(hi[:, rr], lo[:, rr], hi[...], lo[...], 0, 0)
            v_r[s, rr, :] = STAT_DECAY * v_r[s, rr, :] + (1.0 - STAT_DECAY) * right

    def rows_of(s, p, blk):
        r0, rn = AG_ROWS[s][p]
        return dirs.at[blk, pl.ds(r0, rn), :]

    def owner(p, m):
        return flip(me, frame_mask(p, m))

    def hi_bit(m):
        return 4 if m & 4 else (2 if m & 2 else 1)

    def landing(s, p, m, core_of=0):
        if s == 1 and m == 7:
            r0, rn = AG_ROWS[s][p]
            return late.at[core_of, pl.ds(r0, rn), :]
        dev = owner(p, m)
        return rows_of(s, p, 2 * (other_core(dev) if core_of else dev) + s)

    def ag_copy(s, p, m):
        top = hi_bit(m)
        held = m - top
        r0, rn = AG_ROWS[s][p]
        blk = 2 * owner(p, held) + s
        src = dstage.at[s, pl.ds(r0, rn), :] if held == 0 else rows_of(s, p, blk)
        dst = landing(s, p, m) if m == 7 and s == 1 else rows_of(s, p, blk)
        return pltpu.make_async_remote_copy(
            src_ref=src, dst_ref=dst, send_sem=ag_s.at[s], recv_sem=ag_r.at[s, m - 1],
            device_id=(owner(p, top),), device_id_type=MESH)

    def tile_like(s, m, core_of):
        return late.at[core_of] if m == 7 and s == 1 else dirs.at[0]

    def dd_copy(s, p, m):
        ref = landing(s, p, m)
        return pltpu.make_async_remote_copy(
            src_ref=ref, dst_ref=landing(s, p, m, 1) if m == 7 and s == 1 else ref,
            send_sem=dd_s.at[s], recv_sem=dd_r.at[s, m - 1], device_id=(mate,), device_id_type=MESH)

    def dd_wait(s, ms):
        for m in ms:
            wait_all(tile_like(s, m, 1), dd_s.at[s], dd_r.at[s, m - 1]).wait_recv()

    def own_local(s):
        return pltpu.make_async_copy(dstage.at[s], dirs.at[2 * me + s], own_sem.at[s])

    def own_mate(s, recv=False):
        blk = 2 * (mate if recv else me) + s
        return pltpu.make_async_remote_copy(
            src_ref=dstage.at[s], dst_ref=dirs.at[blk], send_sem=do_s.at[s], recv_sem=do_r.at[s],
            device_id=(mate,), device_id_type=MESH)

    def ag_start(s):
        for m in (1, 2, 4):
            for p in range(3):
                ag_copy(s, p, m).start()
        own_mate(s).start()
        own_local(s).start()

    def ag_take(s, ms):
        for m in ms:
            wait_all(tile_like(s, m, 0), ag_s.at[s], ag_r.at[s, m - 1]).wait_recv()
            for nxt in (2, 4):
                if nxt > m:
                    for p in range(3):
                        ag_copy(s, p, m | nxt).start()
            for p in range(3):
                dd_copy(s, p, m).start()

    for j in range(4):
        rs_take(0, j, (4 + j,) if j < 2 else ())
    prep_roots(0)
    prep_roots(1)
    for j in range(4):
        rs_take(1, j)
    rs_take(0, 4, (6,))
    for j in (4, 5):
        for p in range(3):
            rs_copy(1, p, j).start()
    for j in (5, 6):
        rs_take(0, j)
    for n in range(4):
        state_wait(n)
    block_math(0)
    ag_start(0)
    rs_take(1, 4, (6,))
    stats(0)
    rs_take(1, 5)
    ag_take(0, (1, 2))
    rs_take(1, 6)
    block_math(1)
    ag_start(1)

    wait_all(w2v.at[pl.ds(0, 7)], rs_s.at[0], rs_r.at[0, 0]).wait_send()
    w_copies = [
        pltpu.make_async_copy(w1.at[pl.ds(0, B)], w1a, w_sem.at[0]),
        pltpu.make_async_copy(w1.at[pl.ds(B, B)], w1b, w_sem.at[1])]
    w_copies += [pltpu.make_async_copy(w2.at[pl.ds(n * B, B)], w2v.at[n], w_sem.at[2 + n]) for n in range(8)]
    for cp in w_copies:
        cp.start()
    ag_take(0, (3,))
    stats(1)

    def ring(slot):
        return ybuf.at[lax.div(slot, 2), :, span(lax.rem(slot, 2), B)]

    def d_load(blk, slot):
        return pltpu.make_async_copy(dirs.at[blk], ring(slot), db_sem.at[slot])

    def apply_rows(out_ref, c, src):
        cols = span(c, B)

        def rows(rr, _):
            w = out_ref[rr, cols]
            out_ref[rr, cols] = w - LEARN_RATE * (src[rr, :].astype(F32) + WEIGHT_DECAY * w)

        sweep(rows)

    def apply_block(blk, src):
        @pl.when(blk < 8)
        def _():
            apply_rows(w1a, blk, src)

        @pl.when((blk >= 8) & (blk < N_DEV))
        def _():
            apply_rows(w1b, blk - 8, src)

        @pl.when(blk >= N_DEV)
        def _():
            apply_rows(w2v.at[lax.div(blk - N_DEV, 2)], lax.rem(blk, 2), src)

    def apply_range(blk_of, last, early=None, ready=None):
        def load(t):
            t = jnp.int32(t)
            return d_load(blk_of(t), t)

        for t in range(last):
            if t == early:
                ready()
            load(t).start()

        def step(t, _):
            load(t).wait()
            apply_block(blk_of(t), ring(t))
            return 0

        lax.fori_loop(0, last, step, 0)

    def landed(dev, s, t):
        return 2 * move(dev, bits_of(jnp.int32(LANDING[0]), LANDING, t)) + s

    def between(dev):
        return lambda t: landed(dev, jnp.where(t == 0, 0, 1), jnp.where(t == 0, 7, t - 1))

    def sent(s):
        wait_all(dirs.at[pl.ds(0, 7)], ag_s.at[s], ag_r.at[s, 0]).wait_send()
        wait_all(dirs.at[pl.ds(0, 7)], dd_s.at[s], dd_r.at[s, 0]).wait_send()

    ag_take(1, (1, 2))
    for cp in w_copies:
        cp.wait()
    for s in range(2):
        own_local(s).wait()
        own_mate(s).wait_send()
        own_mate(s, True).wait_recv()
    ag_take(0, (4, 5, 6))
    apply_range(lambda t: landed(me, 0, t), 7)
    dd_wait(0, range(1, 7))
    apply_range(lambda t: landed(mate, 0, t), 7)
    ag_take(0, (7,))
    ag_take(1, (4,))
    apply_range(between(me), 5)
    dd_wait(0, (7,))
    dd_wait(1, (1, 2, 4))
    apply_range(between(mate), 5)
    ag_take(1, (3,))
    sent(0)
    ag_take(1, (5, 6))
    apply_range(lambda t: landed(jnp.where(t < 3, me, mate), 1, 4 + lax.rem(t, 3)), 6, 3, lambda: dd_wait(1, (3, 5, 6)))
    ag_take(1, (7,))
    apply_block(landed(me, 1, 7), late.at[0])
    dd_wait(1, (7,))
    apply_block(landed(mate, 1, 7), late.at[1])
    sent(1)


def write_out(w1a, w1b, w2v, v_l, v_r, v_a, v_m, ow1, ow2, o_l, o_r, o_a, o_m, sem):
    pairs = [(v_l, o_l), (v_r, o_r), (v_a, o_a), (v_m, o_m)]
    for n in range(4):
        rr = pl.ds(n * B // 4, B // 4)
        pairs += [(w1a.at[rr], ow1.at[rr]), (w1b.at[rr], ow1.at[pl.ds(B + n * B // 4, B // 4)])]
    pairs += [(w2v.at[n], ow2.at[pl.ds(n * B, B)]) for n in range(8)]
    stores = [pltpu.make_async_copy(src, dst, sem.at[n]) for n, (src, dst) in enumerate(pairs)]
    for cp in stores:
        cp.start()
    for cp in stores:
        cp.wait()


def solution(mesh):
    def per_device(x_in, dy_mid, x_mid, dy_out, w_fc1, w_fc2, stat_left, stat_right, root_left, root_right, graft_sq, momentum):
        vmem = pl.BlockSpec(memory_space=pltpu.VMEM)
        hbm = pl.BlockSpec(memory_space=pltpu.HBM)
        dma = pltpu.SemaphoreType.DMA
        half = pltpu.VMEM((B, w_fc1.shape[1]), F32)
        state = pltpu.VMEM(stat_left.shape, F32)
        tiles = pltpu.VMEM((2, B, B), BF16)
        parts = dma((2, 7))
        pair = dma((2,))
        *done, _ = pl.pallas_call(
            body,
            out_shape=(half, half, pltpu.VMEM((8, B, B2), F32), state, state, state, state, pltpu.HBM((2 * N_DEV, B, B), BF16)),
            in_specs=[hbm] * 12,
            out_specs=(vmem,) * 7 + (hbm,),
            scratch_shapes=[
                pltpu.VMEM((DEPTH, B, B), BF16), pltpu.VMEM((DEPTH, B, B2), BF16), pltpu.VMEM((2, B, B2), F32), tiles, tiles,
                dma((2, DEPTH)), dma((4,)), dma((2, 2)), dma((10,)), pair, dma((RING,)), dma((1,)), dma((2, 2)),
                dma((1,)), parts, pair, parts, pair, parts, pair, pair],
            compiler_params=pltpu.CompilerParams(collective_id=0, has_side_effects=True, vmem_limit_bytes=VMEM_GRANT),
            name='shampoo_step',
        )(x_in, dy_mid, x_mid, dy_out, w_fc1, w_fc2, stat_left, stat_right, root_left, root_right, graft_sq, momentum)
        like = (w_fc1, w_fc2, stat_left, stat_right, graft_sq, momentum)
        return pl.pallas_call(
            write_out,
            out_shape=tuple(jax.ShapeDtypeStruct(v.shape, F32) for v in like),
            in_specs=[vmem] * 7,
            out_specs=(hbm,) * 6,
            scratch_shapes=[dma((20,))],
            compiler_params=pltpu.CompilerParams(vmem_limit_bytes=VMEM_GRANT),
            name='write_out',
        )(*done)

    row_spec = P('dp', None)
    rep_spec = P(None, None)
    tile_spec = P('dp', None, None)
    in_specs = (row_spec, row_spec, row_spec, row_spec, rep_spec, rep_spec, tile_spec, tile_spec, tile_spec, tile_spec, tile_spec, tile_spec)
    out_specs = (rep_spec, rep_spec, tile_spec, tile_spec, tile_spec, tile_spec)
    return jax.shard_map(per_device, mesh=mesh, in_specs=in_specs, out_specs=out_specs, check_vma=False)
```

```python
import functools

import jax
import jax.numpy as jnp
from jax import lax
from jax.experimental import pallas as pl
from jax.experimental.pallas import tpu as pltpu
from jax.sharding import PartitionSpec as P

STEP = 10
STAT_DECAY = 0.999
MOM_DECAY = 0.9
GRAFT_EPS = 1e-8
LEARN_RATE = 0.01
WEIGHT_DECAY = 1e-4
BIAS_CORR = 1.0 - STAT_DECAY ** STEP

MESH = pl.DeviceIdType.MESH
B = 512
B2 = 2 * B
CH = 32
HALF = B // 2
DEPTH = 4
RING = 8
VMEM_GRANT = 12 << 20
N_DEV = 16
ORDER = (7, 3, 5, 6, 1, 2, 4, 0)
LANDING = (0, 1, 2, 4, 3, 5, 6, 7)
AXES = ((1, 2, 4), (2, 4, 1), (4, 1, 2))
RS_ROWS = (((0, 176), (176, 168), (344, 168)), ((0, 168), (168, 176), (344, 168)))
AG_ROWS = (((0, 176), (176, 176), (352, 160)), ((0, 176), (176, 160), (336, 176)))
F32 = jnp.float32
BF16 = jnp.bfloat16


def flip(dev, mask):
    out = dev
    for bit in (1, 2, 4):
        if mask & bit:
            width = 2 * bit
            out = out + width - 2 * width * lax.rem(lax.div(dev, width), 2)
    return out


def other_core(dev):
    return dev + 1 - 2 * lax.rem(dev, 2)


def frame_mask(p, m):
    return sum(AXES[p][i] for i in range(3) if m & (1 << i))


def split(v):
    hi = v.astype(BF16)
    return hi, (v - hi.astype(F32)).astype(BF16)


def dot(a, b, ca, cb):
    return lax.dot_general(a, b, (((ca,), (cb,)), ((), ())), preferred_element_type=F32)


def dot_tn(a, b):
    return dot(a, b, 0, 0)


def dot3(a_hi, a_lo, b_hi, b_lo, ca, cb):
    return dot(a_hi, b_hi, ca, cb) + (dot(a_hi, b_lo, ca, cb) + dot(a_lo, b_hi, ca, cb))


def span(t, size):
    return pl.ds(pl.multiple_of(t * size, size), size)


def sweep(fn, init=None):
    def step(t, carry):
        out = fn(span(t, CH), carry)
        return carry if out is None else out

    return lax.fori_loop(0, B // CH, step, jnp.int32(0) if init is None else init)


def bits_of(rel, table, t):
    for n, value in enumerate(table):
        if n:
            rel = jnp.where(t == n, value, rel)
    return rel


def move(dev, rel):
    out = lax.rem(dev, 2)
    for bit in (1, 2, 4):
        out = out + 2 * bit * lax.rem(lax.div(dev, 2 * bit) + lax.div(rel, bit), 2)
    return out


def apply_to(w1a, w1b, w2v, blk, src):
    def apply_rows(out_ref, c):
        cols = span(c, B)

        def rows(rr, _):
            w = out_ref[rr, cols]
            out_ref[rr, cols] = w - LEARN_RATE * (src[rr, :].astype(F32) + WEIGHT_DECAY * w)

        sweep(rows)

    @pl.when(blk < 8)
    def _():
        apply_rows(w1a, blk)

    @pl.when((blk >= 8) & (blk < N_DEV))
    def _():
        apply_rows(w1b, blk - 8)

    @pl.when(blk >= N_DEV)
    def _():
        apply_rows(w2v.at[lax.div(blk - N_DEV, 2)], lax.rem(blk, 2))


def body(x_in, dy_mid, x_mid, dy_out, w1, w2, st_l, st_r, rt_l, rt_r, gsq, mom,
         w1a, w1b, w2v, v_l, v_r, v_a, v_m, late, dirs,
         xbuf, ybuf, res, dstage,
         op_sem, st_sem, rt_sem, w_sem, own_sem, db_sem, d2d_s, d2d_r, rs_s, rs_r, ag_s, ag_r, dd_s, dd_r, do_s, do_r):
    me = lax.axis_index('dp')
    core = lax.rem(me, 2)
    mate = other_core(me)

    barrier = pltpu.get_barrier_semaphore()
    for nb in (mate, flip(me, 1), flip(me, 2), flip(me, 4)):
        pl.semaphore_signal(barrier, inc=1, device_id=(nb,), device_id_type=MESH)

    def op_start(q):
        h = lax.rem(q, DEPTH)
        side = lax.div(q, DEPTH)
        dest = move(me, bits_of(jnp.int32(ORDER[0]), ORDER, lax.div(side, 2)))
        kd = jnp.where(lax.rem(side, 2) == 0, other_core(dest), dest)
        rows = span(h, B)

        @pl.when(dest < N_DEV // 2)
        def _():
            pltpu.make_async_copy(x_in.at[rows, span(lax.div(kd, 4), B)], xbuf.at[h], op_sem.at[0, h]).start()
            pltpu.make_async_copy(dy_mid.at[rows, span(lax.rem(kd, 4), B2)], ybuf.at[h], op_sem.at[1, h]).start()

        @pl.when(dest >= N_DEV // 2)
        def _():
            pltpu.make_async_copy(x_mid.at[rows, span(kd - N_DEV // 2, B)], xbuf.at[h], op_sem.at[0, h]).start()
            pltpu.make_async_copy(dy_out.at[rows, :], ybuf.at[h], op_sem.at[1, h]).start()

    def op_wait(h):
        pltpu.make_async_copy(x_in.at[pl.ds(0, B), pl.ds(0, B)], xbuf.at[h], op_sem.at[0, h]).wait()
        pltpu.make_async_copy(dy_mid.at[pl.ds(0, B), pl.ds(0, B2)], ybuf.at[h], op_sem.at[1, h]).wait()

    passes = ((0, 0), (1, 0), (0, 1), (1, 1))

    def first_copies(n, h, fn):
        j, s = passes[n]
        kd = flip(me, ORDER[0]) if j else other_core(flip(me, ORDER[0]))
        rows = pl.ds(h * B, B)
        y_to = ybuf.at[h, :, pl.ds(0, B)]

        @pl.when(kd < N_DEV // 2)
        def _():
            fn(pltpu.make_async_copy(x_in.at[rows, span(lax.div(kd, 4), B)], xbuf.at[h], op_sem.at[0, h]))
            fn(pltpu.make_async_copy(dy_mid.at[rows, span(lax.rem(kd, 4) * 2 + s, B)], y_to, op_sem.at[1, h]))

        @pl.when(kd >= N_DEV // 2)
        def _():
            fn(pltpu.make_async_copy(x_mid.at[rows, span(kd - N_DEV // 2, B)], xbuf.at[h], op_sem.at[0, h]))
            fn(pltpu.make_async_copy(dy_out.at[rows, pl.ds(s * B, B)], y_to, op_sem.at[1, h]))

    for h in range(DEPTH):
        first_copies(0, h, lambda cp: cp.start())
    states = ((st_l, v_l), (st_r, v_r), (gsq, v_a), (mom, v_m))
    def acc_at(i, r0, rn, c0, cn):
        return (w1a, w1b)[i // 4].at[pl.ds(r0, rn), pl.ds((i % 4) * B2 + c0, cn)]

    def acc_of(rel, s, p):
        r0, rn = RS_ROWS[s][p]
        return acc_at(ORDER.index(rel), r0, rn, s * B, B)

    def got(s, p, j):
        r0, rn = RS_ROWS[s][p]
        return w2v.at[j, pl.ds(r0, rn), pl.ds(s * B, B)]

    def rs_rel(p, j):
        a1, a2, a3 = AXES[p]
        return (a2 | a3, a2, a3, 0, a3, 0, 0)[j]

    def rs_copy(s, p, j):
        axis = AXES[p][0 if j < 4 else (1 if j < 6 else 2)]
        return pltpu.make_async_remote_copy(
            src_ref=acc_of(rs_rel(p, j) | axis, s, p), dst_ref=got(s, p, j),
            send_sem=rs_s.at[0], recv_sem=rs_r.at[s, j],
            device_id=(flip(me, axis),), device_id_type=MESH)

    def wait_all(ref, send_sem, recv_sem):
        return pltpu.make_async_remote_copy(
            src_ref=ref, dst_ref=ref, send_sem=send_sem, recv_sem=recv_sem, device_id=(mate,), device_id_type=MESH)

    def rs_take(s, j, then=()):
        wait_all(w2v.at[j, :, pl.ds(s * B, B)], rs_s.at[0], rs_r.at[s, j]).wait_recv()
        for p in range(3):
            ref = acc_of(rs_rel(p, j), s, p)
            ref[...] += got(s, p, j)[...]
            for nxt in then:
                rs_copy(s, p, nxt).start()

    def d2d_copy(i, s, half):
        return pltpu.make_async_remote_copy(
            src_ref=res.at[0, :, pl.ds(s * B, B)], dst_ref=half.at[:, span(lax.rem(i, 4) * 2 + s, B)],
            send_sem=d2d_s.at[0], recv_sem=d2d_r.at[s, lax.rem(i, 2)], device_id=(mate,), device_id_type=MESH)

    def on_half(i, fn):
        @pl.when(i < 4)
        def _():
            fn(w1a)

        @pl.when(i >= 4)
        def _():
            fn(w1b)

    def add_mine(i, s, half):
        d2d_copy(i, s, half).wait_recv()
        cols = span(lax.rem(i, 4) * 2 + s, B)

        def add_rows(rr, _):
            half[rr, cols] += res[1, rr, pl.ds(s * B, B)]

        sweep(add_rows)

    def send_on(ii, s):
        for p in range(3):
            for jj in range(4):
                if (rs_rel(p, jj) | AXES[p][0]) == ORDER[ii]:
                    rs_copy(s, p, jj).start()

    for n, (j, s) in enumerate(passes):
        cols = pl.ds(s * B, B)
        for h in range(DEPTH):
            first_copies(n, h, lambda cp: cp.wait())
            prod = dot_tn(xbuf[h], ybuf[h, :, pl.ds(0, B)])
            if h:
                res[j, :, cols] += prod
            else:
                res[j, :, cols] = prod
            if n + 1 < len(passes):
                first_copies(n + 1, h, lambda cp: cp.start())
            elif h < DEPTH - 1:
                op_start(jnp.int32(2 * DEPTH + h))
        if n == 0:
            pl.semaphore_wait(barrier, 4)
        if j == 0:
            d2d_copy(jnp.int32(0), s, w1a).start()
        if n >= 2:
            add_mine(jnp.int32(0), n - 2, w1a)
            send_on(0, n - 2)

    def compute_step(i, _):
        wait_all(res.at[0], d2d_s.at[0], d2d_r.at[0, 0]).wait_send()

        def side(j, _):
            for h in range(DEPTH):
                ahead = (i * 2 + j) * DEPTH + h + DEPTH - 1

                @pl.when(ahead < 2 * 8 * DEPTH)
                def _(ahead=ahead):
                    op_start(ahead)
                op_wait(h)
                if h:
                    res[j] += dot_tn(xbuf[h], ybuf[h])
                else:
                    res[j] = dot_tn(xbuf[h], ybuf[h])

            @pl.when(j == 0)
            def _():
                on_half(i, lambda half: [d2d_copy(i, s, half).start() for s in range(2)])
            return 0

        lax.fori_loop(0, 2, side, 0)
        for s in range(2):
            on_half(i, lambda half, s=s: add_mine(i, s, half))
            for ii in range(1, 7):
                @pl.when(i == ii)
                def _(ii=ii, s=s):
                    send_on(ii, s)
        return 0

    lax.fori_loop(1, 8, compute_step, 0)
    wait_all(res.at[0], d2d_s.at[0], d2d_r.at[0, 0]).wait_send()

    for n, (src, dst) in enumerate(states):
        pltpu.make_async_copy(src, dst, st_sem.at[n]).start()

    def root_half(s, side):
        return res.at[s, :, pl.ds(side * B, B)]

    for s in range(2):
        for side, src in enumerate((rt_l, rt_r)):
            pltpu.make_async_copy(src.at[s], root_half(s, side), rt_sem.at[s, side]).start()

    def root_hi(s, side):
        return ybuf.at[s, :, pl.ds(side * B, B)]

    def root_lo(s, side):
        return ybuf.at[2 + s, :, pl.ds(side * B, B)]

    def g_hi(s):
        return xbuf.at[s]

    def g_lo(s):
        return xbuf.at[2 + s]

    def prep_roots(s):
        for side, src in enumerate((rt_l, rt_r)):
            pltpu.make_async_copy(src.at[s], root_half(s, side), rt_sem.at[s, side]).wait()

        def rows(rr, _):
            for side in range(2):
                root_hi(s, side)[rr, :], root_lo(s, side)[rr, :] = split(root_half(s, side)[rr, :])

        sweep(rows)

    def state_wait(n):
        pltpu.make_async_copy(states[n][0], states[n][1], st_sem.at[n]).wait()

    first_cols = pl.ds(0, B)

    def block_math(s):
        gref = acc_at(ORDER.index(0), 0, B, s * B, B)
        zero = jnp.zeros((8, B), F32)

        def first(rr, tot):
            g = gref[rr, :] * (1.0 / N_DEV)
            g_hi(s)[rr, :], g_lo(s)[rr, :] = split(g)
            sq = STAT_DECAY * v_a[s, rr, :] + (1.0 - STAT_DECAY) * g * g
            v_a[s, rr, :] = sq
            h = g / (jnp.sqrt(sq / BIAS_CORR) + GRAFT_EPS)
            return tot + jnp.sum((h * h).reshape(-1, 8, B), axis=0)

        h_sum = sweep(first, zero)

        def left(t, _):
            rr = span(t, HALF)
            v = dot3(root_hi(s, 0)[rr, :], root_lo(s, 0)[rr, :], g_hi(s)[...], g_lo(s)[...], 1, 0)
            g_hi(1 - s)[rr, :], g_lo(1 - s)[rr, :] = split(v)
            return 0

        lax.fori_loop(0, 2, left, 0)

        def right(t, tot):
            rr = span(t, HALF)
            v = dot3(g_hi(1 - s)[rr, :], g_lo(1 - s)[rr, :], root_hi(s, 1)[...], root_lo(s, 1)[...], 1, 0)
            res[0, rr, first_cols] = v
            return tot + jnp.sum((v * v).reshape(-1, 8, B), axis=0)

        p_sum = lax.fori_loop(0, 2, right, zero)
        ratio = jnp.sqrt(jnp.sum(h_sum, keepdims=True)) / jnp.sqrt(jnp.sum(p_sum, keepdims=True))

        def last(rr, _):
            m = MOM_DECAY * v_m[s, rr, :] + res[0, rr, first_cols] * ratio
            v_m[s, rr, :] = m
            dstage[s, rr, :] = m.astype(BF16)

        sweep(last)

    def stats(s):
        hi, lo = g_hi(s), g_lo(s)
        for t in range(2):
            rr = pl.ds(t * HALF, HALF)
            left = dot3(hi[rr, :], lo[rr, :], hi[...], lo[...], 1, 1)
            v_l[s, rr, :] = STAT_DECAY * v_l[s, rr, :] + (1.0 - STAT_DECAY) * left
            right = dot3(hi[:, rr], lo[:, rr], hi[...], lo[...], 0, 0)
            v_r[s, rr, :] = STAT_DECAY * v_r[s, rr, :] + (1.0 - STAT_DECAY) * right

    def rows_of(s, p, blk):
        r0, rn = AG_ROWS[s][p]
        return dirs.at[blk, pl.ds(r0, rn), :]

    def owner(p, m):
        return flip(me, frame_mask(p, m))

    def hi_bit(m):
        return 4 if m & 4 else (2 if m & 2 else 1)

    def landing(s, p, m, core_of=0):
        if s == 1 and m == 7:
            r0, rn = AG_ROWS[s][p]
            return late.at[core_of, pl.ds(r0, rn), :]
        dev = owner(p, m)
        return rows_of(s, p, 2 * (other_core(dev) if core_of else dev) + s)

    def ag_copy(s, p, m):
        top = hi_bit(m)
        held = m - top
        r0, rn = AG_ROWS[s][p]
        blk = 2 * owner(p, held) + s
        src = dstage.at[s, pl.ds(r0, rn), :] if held == 0 else rows_of(s, p, blk)
        dst = landing(s, p, m) if m == 7 and s == 1 else rows_of(s, p, blk)
        return pltpu.make_async_remote_copy(
            src_ref=src, dst_ref=dst, send_sem=ag_s.at[s], recv_sem=ag_r.at[s, m - 1],
            device_id=(owner(p, top),), device_id_type=MESH)

    def tile_like(s, m, core_of):
        return late.at[core_of] if m == 7 and s == 1 else dirs.at[0]

    def dd_copy(s, p, m):
        ref = landing(s, p, m)
        return pltpu.make_async_remote_copy(
            src_ref=ref, dst_ref=landing(s, p, m, 1) if m == 7 and s == 1 else ref,
            send_sem=dd_s.at[s], recv_sem=dd_r.at[s, m - 1], device_id=(mate,), device_id_type=MESH)

    def dd_wait(s, ms):
        for m in ms:
            wait_all(tile_like(s, m, 1), dd_s.at[s], dd_r.at[s, m - 1]).wait_recv()

    def own_local(s):
        return pltpu.make_async_copy(dstage.at[s], dirs.at[2 * me + s], own_sem.at[s])

    def own_mate(s, recv=False):
        blk = 2 * (mate if recv else me) + s
        return pltpu.make_async_remote_copy(
            src_ref=dstage.at[s], dst_ref=dirs.at[blk], send_sem=do_s.at[s], recv_sem=do_r.at[s],
            device_id=(mate,), device_id_type=MESH)

    def ag_start(s):
        for m in (1, 2, 4):
            for p in range(3):
                ag_copy(s, p, m).start()
        own_mate(s).start()
        own_local(s).start()

    def ag_take(s, ms):
        for m in ms:
            wait_all(tile_like(s, m, 0), ag_s.at[s], ag_r.at[s, m - 1]).wait_recv()
            for nxt in (2, 4):
                if nxt > m:
                    for p in range(3):
                        ag_copy(s, p, m | nxt).start()
            for p in range(3):
                dd_copy(s, p, m).start()

    for j in range(4):
        rs_take(0, j, (4 + j,) if j < 2 else ())
    prep_roots(0)
    prep_roots(1)
    for j in range(4):
        rs_take(1, j)
    rs_take(0, 4, (6,))
    for j in (4, 5):
        for p in range(3):
            rs_copy(1, p, j).start()
    for j in (5, 6):
        rs_take(0, j)
    for n in range(4):
        state_wait(n)
    block_math(0)
    ag_start(0)
    rs_take(1, 4, (6,))
    stats(0)
    rs_take(1, 5)
    ag_take(0, (1, 2))
    rs_take(1, 6)
    block_math(1)
    ag_start(1)

    wait_all(w2v.at[pl.ds(0, 7)], rs_s.at[0], rs_r.at[0, 0]).wait_send()
    w_copies = [
        pltpu.make_async_copy(w1.at[pl.ds(0, B)], w1a, w_sem.at[0]),
        pltpu.make_async_copy(w1.at[pl.ds(B, B)], w1b, w_sem.at[1])]
    w_copies += [pltpu.make_async_copy(w2.at[pl.ds(n * B, B)], w2v.at[n], w_sem.at[2 + n]) for n in range(8)]
    for cp in w_copies:
        cp.start()
    ag_take(0, (3,))
    stats(1)

    def ring(slot):
        return ybuf.at[lax.div(slot, 2), :, span(lax.rem(slot, 2), B)]

    def d_load(blk, slot):
        return pltpu.make_async_copy(dirs.at[blk], ring(slot), db_sem.at[slot])

    def apply_block(blk, src):
        apply_to(w1a, w1b, w2v, blk, src)

    def apply_range(blk_of, last, early=None, ready=None):
        def load(t):
            t = jnp.int32(t)
            return d_load(blk_of(t), t)

        for t in range(last):
            if t == early:
                ready()
            load(t).start()

        def step(t, _):
            load(t).wait()
            apply_block(blk_of(t), ring(t))
            return 0

        lax.fori_loop(0, last, step, 0)

    def landed(dev, s, t):
        return 2 * move(dev, bits_of(jnp.int32(LANDING[0]), LANDING, t)) + s

    def between(dev):
        return lambda t: landed(dev, jnp.where(t == 0, 0, 1), jnp.where(t == 0, 7, t - 1))

    def sent(s):
        wait_all(dirs.at[pl.ds(0, 7)], ag_s.at[s], ag_r.at[s, 0]).wait_send()
        wait_all(dirs.at[pl.ds(0, 7)], dd_s.at[s], dd_r.at[s, 0]).wait_send()

    ag_take(1, (1, 2))
    for cp in w_copies:
        cp.wait()
    for s in range(2):
        own_local(s).wait()
        own_mate(s).wait_send()
        own_mate(s, True).wait_recv()
    ag_take(0, (4, 5, 6))
    apply_range(lambda t: landed(me, 0, t), 7)
    dd_wait(0, range(1, 7))
    apply_range(lambda t: landed(mate, 0, t), 7)
    ag_take(0, (7,))
    ag_take(1, (4,))
    apply_range(between(me), 5)
    dd_wait(0, (7,))
    dd_wait(1, (1, 2, 4))
    apply_range(between(mate), 5)
    ag_take(1, (3,))
    sent(0)
    ag_take(1, (5, 6))
    apply_range(lambda t: landed(jnp.where(t < 3, me, mate), 1, 4 + lax.rem(t, 3)), 6, 3, lambda: dd_wait(1, (3, 5, 6)))
    ag_take(1, (7,))
    dd_wait(1, (7,))
    sent(1)


def write_out(w1a, w1b, w2v, v_l, v_r, v_a, v_m, late, ow1, ow2, o_l, o_r, o_a, o_m, sem):
    far = flip(lax.axis_index('dp'), 7)
    first = 2 * far + 1
    states = [(v_l, o_l), (v_r, o_r), (v_a, o_a), (v_m, o_m)]
    spans = [pl.ds(n * B // 4, B // 4) for n in range(4)]
    upper = [(w1a.at[rr], ow1.at[rr]) for rr in spans]
    lower = [(w1b.at[rr], ow1.at[pl.ds(B + n * B // 4, B // 4)]) for n, rr in enumerate(spans)]
    second = [(w2v.at[n], ow2.at[pl.ds(n * B, B)]) for n in range(8)]
    pairs = states + upper + lower + second
    stores = [pltpu.make_async_copy(src, dst, sem.at[n]) for n, (src, dst) in enumerate(pairs)]

    def go(lo, hi, when):
        @pl.when(when)
        def _():
            for cp in stores[lo:hi]:
                cp.start()

    regions = ((4, 8, first < 8), (8, 12, (first >= 8) & (first < N_DEV)), (12, 20, first >= N_DEV))
    for cp in stores[:4]:
        cp.start()
    for lo, hi, held in regions:
        go(lo, hi, jnp.logical_not(held))
    apply_to(w1a, w1b, w2v, first, late.at[0])
    apply_to(w1a, w1b, w2v, 2 * other_core(far) + 1, late.at[1])
    for lo, hi, held in regions:
        go(lo, hi, held)
    for cp in stores:
        cp.wait()


def solution(mesh):
    def per_device(x_in, dy_mid, x_mid, dy_out, w_fc1, w_fc2, stat_left, stat_right, root_left, root_right, graft_sq, momentum):
        vmem = pl.BlockSpec(memory_space=pltpu.VMEM)
        hbm = pl.BlockSpec(memory_space=pltpu.HBM)
        dma = pltpu.SemaphoreType.DMA
        half = pltpu.VMEM((B, w_fc1.shape[1]), F32)
        state = pltpu.VMEM(stat_left.shape, F32)
        tiles = pltpu.VMEM((2, B, B), BF16)
        parts = dma((2, 7))
        pair = dma((2,))
        *done, _ = pl.pallas_call(
            body,
            out_shape=(half, half, pltpu.VMEM((8, B, B2), F32), state, state, state, state, tiles, pltpu.HBM((2 * N_DEV, B, B), BF16)),
            in_specs=[hbm] * 12,
            out_specs=(vmem,) * 8 + (hbm,),
            scratch_shapes=[
                pltpu.VMEM((DEPTH, B, B), BF16), pltpu.VMEM((DEPTH, B, B2), BF16), pltpu.VMEM((2, B, B2), F32), tiles,
                dma((2, DEPTH)), dma((4,)), dma((2, 2)), dma((10,)), pair, dma((RING,)), dma((1,)), dma((2, 2)),
                dma((1,)), parts, pair, parts, pair, parts, pair, pair],
            compiler_params=pltpu.CompilerParams(collective_id=0, has_side_effects=True, vmem_limit_bytes=VMEM_GRANT),
            name='shampoo_step',
        )(x_in, dy_mid, x_mid, dy_out, w_fc1, w_fc2, stat_left, stat_right, root_left, root_right, graft_sq, momentum)
        like = (w_fc1, w_fc2, stat_left, stat_right, graft_sq, momentum)
        return pl.pallas_call(
            write_out,
            out_shape=tuple(jax.ShapeDtypeStruct(v.shape, F32) for v in like),
            in_specs=[vmem] * 8,
            out_specs=(hbm,) * 6,
            scratch_shapes=[dma((20,))],
            compiler_params=pltpu.CompilerParams(vmem_limit_bytes=VMEM_GRANT),
            name='write_out',
        )(*done)

    row_spec = P('dp', None)
    rep_spec = P(None, None)
    tile_spec = P('dp', None, None)
    in_specs = (row_spec, row_spec, row_spec, row_spec, rep_spec, rep_spec, tile_spec, tile_spec, tile_spec, tile_spec, tile_spec, tile_spec)
    out_specs = (rep_spec, rep_spec, tile_spec, tile_spec, tile_spec, tile_spec)
    return jax.shard_map(per_device, mesh=mesh, in_specs=in_specs, out_specs=out_specs, check_vma=False)
```
